32 devices in a mesh: dp: 1 (over z), pool: 4 (over y), ep: 8 (over x, core).
Axes of the slice: x: 4, y: 4, z: 1, core: 2. Of those that a mesh axis runs over, the one named last changes fastest.
The devices are a block of a 4x4x8 slice.
Arguments:
- x: bfloat16 [2048, 1536], P(('dp', 'ep', 'pool'))
- k_cache: bfloat16 [2, 2048, 128, 2, 128], P(None, ('dp', 'ep'))
- v_cache: bfloat16 [2, 2048, 128, 2, 128], P(None, ('dp', 'ep'))
- cache_len: int32 [2048], P(('dp', 'ep'))
- w_query: bfloat16 [2, 1536, 1536], replicated
- w_key: bfloat16 [2, 1536, 256], replicated
- w_value: bfloat16 [2, 1536, 256], replicated
- w_out: bfloat16 [2, 1536, 1536], replicated
- w_router: float32 [2, 1536, 8], replicated
- expert_ids: int32 [2, 2048, 2], P(None, ('dp', 'ep'))
- w_gate: bfloat16 [2, 8, 1536, 4096], P(None, 'ep')
- w_up: bfloat16 [2, 8, 1536, 4096], P(None, 'ep')
- w_down: bfloat16 [2, 8, 4096, 1536], P(None, 'ep')
- shared_gate: bfloat16 [2, 1536, 4096], replicated
- shared_up: bfloat16 [2, 1536, 4096], replicated
- shared_down: bfloat16 [2, 4096, 1536], replicated
Outputs:
- output: bfloat16 [2048, 1536], P(('dp', 'ep', 'pool'))
All inputs are finite; a program needn't handle non-finite values.
Results may differ from the reference program's by a relative error of at most 0.0184699.
Values are sent between devices in bfloat16 or wider.
A program may use at most 768 MiB of HBM per device.

```python
import math
import jax
import jax.numpy as jnp
from jax import lax

TOK_DEV = 64
CTX_LEN = 128
D_MODEL = 1536
Q_HEADS = 12
KV_HEADS = 2
HEAD_DIM = 128
EXPERTS = 8
TOP_K = 2
EXPERT_FF = 4096
SHARED_FF = 4096
N_LAYERS = 2
EP_SIZE = 8
POOL_SIZE = 4
ROPE_BASE = 10000
RMS_EPS = 1e-6
HALF_POOL = POOL_SIZE // 2
BATCH = EP_SIZE * POOL_SIZE * TOK_DEV
GROUP_TOK = 2 * TOK_DEV
CAPACITY = 3 * TOK_DEV * TOP_K // EP_SIZE
EXP_LOCAL = EXPERTS // EP_SIZE
CTX_BITS = int(math.log2(CTX_LEN))


def draw_normal(key, shape, scale):
    return (jax.random.normal(key, shape, jnp.float32) * scale).astype(jnp.bfloat16)


def draw_lengths(key):
    key_a, key_b, key_c = jax.random.split(key, 3)
    level = jax.random.randint(key_a, (BATCH,), 0, CTX_BITS + 1)
    low = jnp.left_shift(jnp.ones_like(level), level)
    lens = jnp.minimum(low + jax.random.randint(key_b, (BATCH,), 0, low), CTX_LEN)
    return lens.at[jax.random.randint(key_c, (), 0, BATCH)].set(CTX_LEN)


def draw_routing(key):
    keys = jax.random.split(key, 3)
    groups = N_LAYERS * EP_SIZE * HALF_POOL
    pairs = GROUP_TOK * TOP_K
    rest = pairs - CAPACITY
    hot_dev = jax.random.randint(keys[0], (groups, 1), 0, EP_SIZE)
    dev_idx = jnp.arange(EP_SIZE)[None, :]
    other_rank = (dev_idx - hot_dev - 1) % EP_SIZE
    counts = jnp.where(dev_idx == hot_dev, CAPACITY, rest // (EP_SIZE - 1) + (other_rank < rest % (EP_SIZE - 1)).astype(jnp.int32))
    ends = jnp.cumsum(counts, axis=1)
    starts = ends - counts
    pair_idx = jnp.arange(pairs)
    dev_of = jnp.sum((pair_idx[None, :, None] >= ends[:, None, :]).astype(jnp.int32), axis=2)
    start_of = jnp.take_along_axis(starts, dev_of, axis=1)
    shifts = jax.random.randint(keys[1], (groups, EP_SIZE), 0, EXP_LOCAL)
    local_of = ((pair_idx[None, :] - start_of) // GROUP_TOK + jnp.take_along_axis(shifts, dev_of, axis=1)) % EXP_LOCAL
    by_choice = (dev_of * EXP_LOCAL + local_of).reshape(groups, TOP_K, GROUP_TOK)
    scores = jax.random.randint(keys[2], (groups, GROUP_TOK), 0, 1 << 20) * GROUP_TOK + jnp.arange(GROUP_TOK)[None, :]
    token_perm = jnp.argsort(scores, axis=1)
    picked = jnp.take_along_axis(by_choice, token_perm[:, None, :], axis=2)
    picked = picked.reshape(N_LAYERS, EP_SIZE, HALF_POOL, TOP_K, 2, TOK_DEV)
    return picked.transpose(0, 1, 4, 2, 5, 3).reshape(N_LAYERS, BATCH, TOP_K)


def setup_inputs(seed: int = 0, part: int = 0) -> dict:
    part_keys = jax.random.split(jax.random.fold_in(jax.random.key(seed), part), 5)
    weight_keys = jax.random.split(jax.random.key(seed + 1), 12)
    inner_dim = Q_HEADS * HEAD_DIM
    cache_shape = (N_LAYERS, BATCH, CTX_LEN, KV_HEADS, HEAD_DIM)
    return {
        "x": draw_normal(part_keys[0], (BATCH, D_MODEL), 1.0),
        "k_cache": draw_normal(part_keys[1], cache_shape, 1.0),
        "v_cache": draw_normal(part_keys[2], cache_shape, 1.0),
        "cache_len": draw_lengths(part_keys[3]),
        "w_query": draw_normal(weight_keys[0], (N_LAYERS, D_MODEL, inner_dim), D_MODEL ** -0.5),
        "w_key": draw_normal(weight_keys[1], (N_LAYERS, D_MODEL, KV_HEADS * HEAD_DIM), D_MODEL ** -0.5),
        "w_value": draw_normal(weight_keys[2], (N_LAYERS, D_MODEL, KV_HEADS * HEAD_DIM), D_MODEL ** -0.5),
        "w_out": draw_normal(weight_keys[3], (N_LAYERS, inner_dim, D_MODEL), 3.0 * inner_dim ** -0.5),
        "w_router": jax.random.normal(weight_keys[4], (N_LAYERS, D_MODEL, EXPERTS), jnp.float32) * (2.0 * D_MODEL ** -0.5),
        "expert_ids": draw_routing(part_keys[4]),
        "w_gate": draw_normal(weight_keys[5], (N_LAYERS, EXPERTS, D_MODEL, EXPERT_FF), D_MODEL ** -0.5),
        "w_up": draw_normal(weight_keys[6], (N_LAYERS, EXPERTS, D_MODEL, EXPERT_FF), D_MODEL ** -0.5),
        "w_down": draw_normal(weight_keys[7], (N_LAYERS, EXPERTS, EXPERT_FF, D_MODEL), 2.0 * EXPERT_FF ** -0.5),
        "shared_gate": draw_normal(weight_keys[8], (N_LAYERS, D_MODEL, SHARED_FF), D_MODEL ** -0.5),
        "shared_up": draw_normal(weight_keys[9], (N_LAYERS, D_MODEL, SHARED_FF), D_MODEL ** -0.5),
        "shared_down": draw_normal(weight_keys[10], (N_LAYERS, SHARED_FF, D_MODEL), SHARED_FF ** -0.5),
    }


def rms_norm(vals):
    flt = vals.astype(jnp.float32)
    return flt * lax.rsqrt(jnp.mean(flt * flt, axis=-1, keepdims=True) + RMS_EPS)


def rotate(vals, pos):
    half = HEAD_DIM // 2
    inv_freq = jnp.exp(jnp.arange(half, dtype=jnp.float32) * (-math.log(ROPE_BASE) / half))
    angle = pos.astype(jnp.float32)[:, None, None] * inv_freq
    cosine = jnp.cos(angle)
    sine = jnp.sin(angle)
    first = vals[..., :half]
    second = vals[..., half:]
    return jnp.concatenate([first * cosine - second * sine, second * cosine + first * sine], axis=-1)


def layer_step(state, cache_len, layer_args):
    (k_layer, v_layer, w_query, w_key, w_value, w_out, w_router, choice_ids, w_gate, w_up, w_down, shared_gate, shared_up, shared_down) = layer_args
    hidden = rms_norm(state).astype(jnp.bfloat16)
    query = jnp.dot(hidden, w_query, preferred_element_type=jnp.float32).reshape(BATCH, Q_HEADS, HEAD_DIM)
    key_new = jnp.dot(hidden, w_key, preferred_element_type=jnp.float32).reshape(BATCH, KV_HEADS, HEAD_DIM)
    val_new = jnp.dot(hidden, w_value, preferred_element_type=jnp.float32).astype(jnp.bfloat16).reshape(BATCH, KV_HEADS, HEAD_DIM)
    query = rotate(query, cache_len).astype(jnp.bfloat16).reshape(BATCH, KV_HEADS, Q_HEADS // KV_HEADS, HEAD_DIM).astype(jnp.float32)
    key_new = rotate(key_new, cache_len).astype(jnp.bfloat16).astype(jnp.float32)
    scale = HEAD_DIM ** -0.5
    s_cache = jnp.einsum("nkgd,nskd->nkgs", query, k_layer.astype(jnp.float32)) * scale
    s_new = jnp.einsum("nkgd,nkd->nkg", query, key_new) * scale
    valid = jnp.arange(CTX_LEN)[None, None, None, :] < cache_len[:, None, None, None]
    s_cache = jnp.where(valid, s_cache, -jnp.inf)
    peak_val = jnp.maximum(jnp.max(s_cache, axis=-1), s_new)
    e_cache = jnp.exp(s_cache - peak_val[..., None])
    e_new = jnp.exp(s_new - peak_val)
    total_exp = jnp.sum(e_cache, axis=-1) + e_new
    p_cache = (e_cache / total_exp[..., None]).astype(jnp.bfloat16).astype(jnp.float32)
    p_new = (e_new / total_exp).astype(jnp.bfloat16).astype(jnp.float32)
    mixed = jnp.einsum("nkgs,nskd->nkgd", p_cache, v_layer.astype(jnp.float32))
    mixed = mixed + p_new[..., None] * val_new.astype(jnp.float32)[:, :, None, :]
    attn = mixed.astype(jnp.bfloat16).reshape(BATCH, Q_HEADS * HEAD_DIM)
    resid = (state.astype(jnp.float32) + jnp.dot(attn, w_out, preferred_element_type=jnp.float32)).astype(jnp.bfloat16)
    normed = rms_norm(resid).astype(jnp.bfloat16)
    logits = jnp.dot(normed.astype(jnp.float32), w_router)
    gates = jax.nn.softmax(jnp.take_along_axis(logits, choice_ids, axis=1), axis=-1)
    flat_ids = choice_ids.reshape(-1)
    order = jnp.argsort(flat_ids, stable=True)
    inverse = jnp.argsort(order, stable=True)
    rows = jnp.take(normed, order // TOP_K, axis=0).astype(jnp.float32)
    sizes = jnp.bincount(flat_ids, length=EXPERTS).astype(jnp.int32)
    gate_part = lax.ragged_dot(rows, w_gate.astype(jnp.float32), sizes)
    up_part = lax.ragged_dot(rows, w_up.astype(jnp.float32), sizes)
    mid = (jax.nn.silu(gate_part) * up_part).astype(jnp.bfloat16).astype(jnp.float32)
    out_sorted = lax.ragged_dot(mid, w_down.astype(jnp.float32), sizes).astype(jnp.bfloat16)
    pair_out = jnp.take(out_sorted, inverse, axis=0).reshape(BATCH, TOP_K, D_MODEL).astype(jnp.float32)
    routed = jnp.sum(gates[..., None] * pair_out, axis=1)
    shared_mid = (jax.nn.silu(jnp.dot(normed, shared_gate, preferred_element_type=jnp.float32)) * jnp.dot(normed, shared_up, preferred_element_type=jnp.float32)).astype(jnp.bfloat16)
    shared_out = jnp.dot(shared_mid, shared_down, preferred_element_type=jnp.float32).astype(jnp.bfloat16)
    return (resid.astype(jnp.float32) + routed + shared_out.astype(jnp.float32)).astype(jnp.bfloat16)


def reference(x, k_cache, v_cache, cache_len, w_query, w_key, w_value, w_out, w_router, expert_ids, w_gate, w_up, w_down, shared_gate, shared_up, shared_down):
    def one_layer(state, layer_args):
        return layer_step(state, cache_len, layer_args), None
    final_x, scan_rest = lax.scan(one_layer, x, (k_cache, v_cache, w_query, w_key, w_value, w_out, w_router, expert_ids, w_gate, w_up, w_down, shared_gate, shared_up, shared_down))
    return final_x
```

```python
import functools
import math
import jax
import jax.numpy as jnp
from jax import lax
from jax.experimental import pallas as pl
from jax.experimental.pallas import tpu as pltpu
from jax.sharding import PartitionSpec as P

RMS_EPS = 1e-6
ROPE_BASE = 10000.0
MESH = pl.DeviceIdType.MESH
BF16 = jnp.bfloat16
F32 = jnp.float32
ANY = pl.BlockSpec(memory_space=pl.ANY)
VMEM = pl.BlockSpec(memory_space=pltpu.VMEM)
SMEM = pl.BlockSpec(memory_space=pltpu.SMEM)
VMEM_BYTES = 66_000_000
META = 128
TOK_STEP = 8
FF_CHUNK = 512
RING = 8


def rms(vals):
    return vals * lax.rsqrt(jnp.mean(vals * vals, axis=-1, keepdims=True) + RMS_EPS)


def mm(lhs, rhs):
    return jnp.dot(lhs, rhs, preferred_element_type=F32)


def silu(vals):
    return vals * (1.0 / (1.0 + jnp.exp(-vals)))


def attention_kernel(layer, capacity, q_heads, kv_heads, lens, x_ref, cos_ref, sin_ref, ids_ref, wr_ref, wq, wk, wv, wo, kc, vc,
                     a_ref, u_ref, meta_ref, wq_b, wk_b, wv_b, wo_b, k_b, v_b, q3, kn3, vn3, o3, attn, w_sem, k_sem, v_sem):
    n_tok, d_model = x_ref.shape
    rows = kc.shape[2]
    head_dim = kc.shape[3]
    group = q_heads // kv_heads
    steps = n_tok // TOK_STEP
    first = lax.axis_index("pool") * n_tok
    scale = head_dim ** -0.5
    weights = [(wq, wq_b), (wk, wk_b), (wv, wv_b), (wo, wo_b)]
    w_copies = [pltpu.make_async_copy(src.at[layer], dst, w_sem.at[i]) for i, (src, dst) in enumerate(weights)]

    def cache_copies(step):
        here = pl.ds(step * TOK_STEP, TOK_STEP)
        there = pl.ds(first + step * TOK_STEP, TOK_STEP)
        return (pltpu.make_async_copy(kc.at[layer, there], k_b.at[here], k_sem.at[step]),
                pltpu.make_async_copy(vc.at[layer, there], v_b.at[here], v_sem.at[step]))

    for copy in w_copies[:3]:
        copy.start()
    for step in range(steps):
        for copy in cache_copies(step):
            copy.start()
    w_copies[3].start()

    q3[...] = jnp.zeros_like(q3)
    kn3[...] = jnp.zeros_like(kn3)
    vn3[...] = jnp.zeros_like(vn3)
    x_f = x_ref[...].astype(F32)
    hidden = rms(x_f).astype(BF16)
    cosine = cos_ref[...]
    sine = sin_ref[...]

    def rotated(vals):
        return (vals * cosine + pltpu.roll(vals, head_dim // 2, 1) * sine).astype(BF16).astype(F32)

    w_copies[0].wait()
    query = mm(hidden, wq_b[...])
    for head in range(q_heads):
        q3[:, head, :] = rotated(query[:, head * head_dim:(head + 1) * head_dim])
    w_copies[1].wait()
    key = mm(hidden, wk_b[...])
    w_copies[2].wait()
    val = mm(hidden, wv_b[...]).astype(BF16).astype(F32)
    for kv in range(kv_heads):
        cols = slice(kv * head_dim, (kv + 1) * head_dim)
        key_rot = rotated(key[:, cols])
        for head in range(kv * group, (kv + 1) * group):
            kn3[:, head, :] = key_rot
            vn3[:, head, :] = val[:, cols]

    pad = q3.shape[1]
    lane = lax.broadcasted_iota(jnp.int32, (pad, rows), 1)
    head_kv = lax.broadcasted_iota(jnp.int32, (pad, rows), 0) // group
    right_kv = lane % kv_heads == head_kv
    position = lane // kv_heads

    def step_body(step, carry):
        for copy in cache_copies(step):
            copy.wait()
        base = step * TOK_STEP
        q_f = q3[pl.ds(base, TOK_STEP)]
        scores = lax.dot_general(q_f.astype(BF16), k_b[pl.ds(base, TOK_STEP)], (((2,), (2,)), ((0,), (0,))), preferred_element_type=F32)
        s_new = jnp.sum(q_f * kn3[pl.ds(base, TOK_STEP)], axis=-1, keepdims=True) * scale
        probs = []
        p_news = []
        for i in range(TOK_STEP):
            valid = right_kv & (position < lens[base + i])
            s_i = jnp.where(valid, scores[i] * scale, -jnp.inf)
            peak = jnp.maximum(jnp.max(s_i, axis=-1, keepdims=True), s_new[i])
            e_i = jnp.exp(s_i - peak)
            e_new = jnp.exp(s_new[i] - peak)
            total = jnp.sum(e_i, axis=-1, keepdims=True) + e_new
            probs.append((e_i / total).astype(BF16))
            p_news.append((e_new / total).astype(BF16).astype(F32))
        for i in range(TOK_STEP):
            mixed = mm(probs[i], v_b[base + i])
            o3[base + i] = mixed + p_news[i] * vn3[base + i]
        return carry

    lax.fori_loop(0, steps, step_body, 0)
    for head in range(q_heads):
        attn[:, head * head_dim:(head + 1) * head_dim] = o3[:, head, :].astype(BF16)
    w_copies[3].wait()
    resid = (x_f + mm(attn[...], wo_b[...])).astype(BF16)
    a_ref[...] = resid
    normed = rms(resid.astype(F32)).astype(BF16)
    u_ref[:, :d_model] = normed

    logits = lax.dot_general(normed.astype(F32), wr_ref[...], (((1,), (1,)), ((), ())), precision=lax.Precision.HIGHEST, preferred_element_type=F32)
    experts = logits.shape[1]
    lane_e = lax.broadcasted_iota(jnp.int32, (n_tok, META), 1)
    id0 = ids_ref[:, 0:1]
    id1 = ids_ref[:, 1:2]
    pick0 = lane_e == id0
    pick1 = lane_e == id1
    l0 = jnp.sum(jnp.where(pick0[:, :experts], logits, 0.0), axis=-1, keepdims=True)
    l1 = jnp.sum(jnp.where(pick1[:, :experts], logits, 0.0), axis=-1, keepdims=True)
    peak = jnp.maximum(l0, l1)
    e0 = jnp.exp(l0 - peak)
    e1 = jnp.exp(l1 - peak)
    member = jnp.where(pick0 | pick1, 1.0, 0.0)
    earlier = jnp.where(lax.broadcasted_iota(jnp.int32, (n_tok, n_tok), 1) < lax.broadcasted_iota(jnp.int32, (n_tok, n_tok), 0), 1.0, 0.0)
    rank = mm(earlier.astype(BF16), member.astype(BF16))
    u_ref[:, d_model:] = jnp.where(member > 0.0, rank, -1.0).astype(BF16)
    slot0 = id0.astype(F32) * capacity + jnp.sum(jnp.where(pick0, rank, 0.0), axis=-1, keepdims=True)
    slot1 = id1.astype(F32) * capacity + jnp.sum(jnp.where(pick1, rank, 0.0), axis=-1, keepdims=True)
    total = e0 + e1
    meta_ref[...] = jnp.where(lane_e == 0, slot0, jnp.where(lane_e == 1, slot1, jnp.where(lane_e == 2, e0 / total, e1 / total)))


def moe_kernel(layer, capacity, ep_size, u_ref, a_ref, meta_ref, sg, su, sd, wg, wu, wd, out_ref,
               gath, back, picked, sent, acc_e, acc_s, g_b, u_b, d_b, w_sem, ag_send, ag_recv, ret_send, ret_recv):
    n_tok = a_ref.shape[0]
    d_model = a_ref.shape[1]
    half = n_tok // 2
    n_chunks = sg.shape[2] // FF_CHUNK
    me = lax.axis_index("ep")
    partner = me + 1 - 2 * lax.rem(me, 2)
    right = lax.rem(me + 2, ep_size)
    left = lax.rem(me + ep_size - 2, ep_size)
    far = lax.rem(me + ep_size // 2, ep_size)

    def weight_copies(chunk, slot, shared):
        cols = pl.ds(chunk * FF_CHUNK, FF_CHUNK)
        if shared:
            srcs = (sg.at[layer, :, cols], su.at[layer, :, cols], sd.at[layer, cols])
        else:
            srcs = (wg.at[layer, 0, :, cols], wu.at[layer, 0, :, cols], wd.at[layer, 0, cols])
        dsts = (g_b.at[slot], u_b.at[slot], d_b.at[slot])
        return [pltpu.make_async_copy(src, dst, w_sem.at[slot, i]) for i, (src, dst) in enumerate(zip(srcs, dsts))]

    for chunk in range(RING):
        for copy in weight_copies(chunk, chunk, True):
            copy.start()

    barrier = pltpu.get_barrier_semaphore()
    for other in range(1, ep_size):
        pl.semaphore_signal(barrier, inc=1, device_id={"ep": lax.rem(me + other, ep_size)}, device_id_type=MESH)
    gath[me] = u_ref[...]
    pl.semaphore_wait(barrier, ep_size - 1)

    def piece(src, part):
        return gath.at[src, pl.ds(part * half, half)]

    def gather_copy(src, part, where, target, from_input=False):
        ref = u_ref.at[pl.ds(part * half, half)] if from_input else piece(src, part)
        return pltpu.make_async_remote_copy(src_ref=ref, dst_ref=piece(src, part), send_sem=ag_send.at[where], recv_sem=ag_recv.at[src, part],
                                            device_id={"ep": target}, device_id_type=MESH)

    def arrived(src, part):
        pltpu.make_async_remote_copy(src_ref=piece(src, part), dst_ref=piece(src, part), send_sem=ag_send.at[0], recv_sem=ag_recv.at[src, part],
                                     device_id={"ep": partner}, device_id_type=MESH).wait_recv()

    sends = []

    def send(src, part, target, from_input=False):
        copy = gather_copy(src, part, len(sends), target, from_input)
        copy.start()
        sends.append(copy)

    send(me, 0, right, True)
    send(me, 1, left, True)
    send(me, 1, right, True)
    send(me, 0, left, True)
    send(me, 0, partner, True)
    send(me, 1, partner, True)

    acc_s[...] = jnp.zeros_like(acc_s)
    acc_e[...] = jnp.zeros_like(acc_e)

    def chunk_mlp(rows, slot):
        mid = (silu(mm(rows, g_b[slot])) * mm(rows, u_b[slot])).astype(BF16)
        return mm(mid, d_b[slot])

    def shared_step(chunk, carry):
        slot = lax.rem(chunk, RING)
        for copy in weight_copies(chunk, slot, True):
            copy.wait()
        acc_s[...] += chunk_mlp(u_ref[:, :d_model], slot)
        for copy in weight_copies(chunk, slot, False):
            copy.start()
        return carry

    lax.fori_loop(0, 3, shared_step, 0)
    arrived(left, 0)
    send(left, 0, right)
    arrived(right, 1)
    send(right, 1, left)
    send(left, 0, partner)
    send(right, 1, partner)
    lax.fori_loop(3, 5, shared_step, 0)
    for src, part in ((left, 1), (right, 0)):
        arrived(src, part)
        send(src, part, partner)
    lax.fori_loop(5, 7, shared_step, 0)
    for src, part in ((far, 0), (far, 1)):
        arrived(src, part)
        send(src, part, partner)
    lax.fori_loop(7, n_chunks, shared_step, 0)
    for hop in (0, 2, ep_size - 2, ep_size // 2):
        for part in (0, 1):
            arrived(lax.rem(partner + hop, ep_size), part)

    lane = lax.broadcasted_iota(jnp.int32, (n_tok, META), 1)

    def pick_step(src, carry):
        codes = gath[src, :, d_model:].astype(F32)
        rank = jnp.sum(jnp.where(lane == me, codes, 0.0), axis=-1, keepdims=True)
        choose = jnp.where(lane.astype(F32) == rank, 1.0, 0.0).astype(BF16)
        rows = lax.dot_general(choose, gath[src, :, :d_model], (((0,), (0,)), ((), ())), preferred_element_type=F32)
        picked[pl.ds(src * capacity, capacity)] = rows[:capacity].astype(BF16)
        return carry

    lax.fori_loop(0, ep_size, pick_step, 0)

    def expert_step(chunk, carry):
        slot = lax.rem(chunk, RING)
        for copy in weight_copies(chunk, slot, False):
            copy.wait()
        acc_e[...] += chunk_mlp(picked[...], slot)
        return carry

    lax.fori_loop(0, n_chunks, expert_step, 0)
    for src in range(ep_size):
        sent[src] = acc_e[pl.ds(src * capacity, capacity)].astype(BF16)

    def return_copy(hop):
        target = lax.rem(me + hop, ep_size)
        return pltpu.make_async_remote_copy(src_ref=sent.at[target], dst_ref=back.at[me], send_sem=ret_send.at[hop], recv_sem=ret_recv.at[me],
                                            device_id={"ep": target}, device_id_type=MESH)

    order = [ep_size // 2, ep_size // 2 + 1, 2, 3, ep_size - 2, ep_size - 1, 1]
    for hop in order:
        return_copy(hop).start()
    back[me] = sent[me]
    for copy in sends:
        copy.wait_send()
    for hop in order:
        return_copy(hop).wait_send()
        src = lax.rem(me + hop, ep_size)
        pltpu.make_async_remote_copy(src_ref=back.at[src], dst_ref=back.at[src], send_sem=ret_send.at[hop], recv_sem=ret_recv.at[src],
                                     device_id={"ep": src}, device_id_type=MESH).wait_recv()

    slot_lane = lax.broadcasted_iota(jnp.int32, (n_tok, ep_size * capacity), 1).astype(F32)
    table = back[...].reshape(ep_size * capacity, d_model)
    y0 = mm(jnp.where(slot_lane == meta_ref[:, 0:1], 1.0, 0.0).astype(BF16), table)
    y1 = mm(jnp.where(slot_lane == meta_ref[:, 1:2], 1.0, 0.0).astype(BF16), table)
    routed = meta_ref[:, 2:3] * y0 + meta_ref[:, 3:4] * y1
    out_ref[...] = (a_ref[...].astype(F32) + routed + acc_s[...].astype(BF16).astype(F32)).astype(BF16)


def solution(mesh):
    ep_size = mesh.shape["ep"]
    row_spec = P(("dp", "ep", "pool"), None)
    cache_spec = P(None, ("dp", "ep"), None, None, None)
    expert_spec = P(None, "ep", None, None)
    in_specs = (row_spec, cache_spec, cache_spec, P(("dp", "ep")), P(), P(), P(), P(), P(), P(None, ("dp", "ep"), None), expert_spec, expert_spec, expert_spec, P(), P(), P())

    def body(x_loc, k_cache, v_cache, cache_len, w_query, w_key, w_value, w_out, w_router, expert_ids, w_gate, w_up, w_down, shared_gate, shared_up, shared_down):
        n_tok, d_model = x_loc.shape
        n_layers, all_tok, ctx, kv_heads, head_dim = k_cache.shape
        q_heads = w_query.shape[2] // head_dim
        top_k = expert_ids.shape[2]
        capacity = 3 * n_tok * top_k // ep_size
        rows = ctx * kv_heads
        pad_heads = -(-q_heads // 8) * 8
        first = lax.axis_index("pool") * n_tok
        lens = lax.dynamic_slice_in_dim(cache_len, first, n_tok, 0)
        ids = lax.dynamic_slice_in_dim(expert_ids, first, n_tok, 1)
        half = head_dim // 2
        inv_freq = jnp.exp(jnp.arange(half, dtype=F32) * (-math.log(ROPE_BASE) / half))
        angle = lens.astype(F32)[:, None] * inv_freq
        cosine = jnp.cos(angle)
        sine = jnp.sin(angle)
        cos2 = jnp.concatenate([cosine, cosine], axis=1)
        sin2 = jnp.concatenate([-sine, sine], axis=1)
        router_t = jnp.swapaxes(w_router, 1, 2)
        k_rows = k_cache.reshape(n_layers, all_tok, rows, head_dim)
        v_rows = v_cache.reshape(n_layers, all_tok, rows, head_dim)
        ext = d_model + META
        x_cur = x_loc
        for layer in range(n_layers):
            resid, u_ext, meta = pl.pallas_call(
                functools.partial(attention_kernel, layer, capacity, q_heads, kv_heads),
                name=f"attention_{layer}",
                out_shape=(jax.ShapeDtypeStruct((n_tok, d_model), BF16), jax.ShapeDtypeStruct((n_tok, ext), BF16), jax.ShapeDtypeStruct((n_tok, META), F32)),
                in_specs=[SMEM] + [VMEM] * 5 + [ANY] * 6,
                out_specs=(VMEM, VMEM, VMEM),
                scratch_shapes=[
                    pltpu.VMEM(w_query.shape[1:], BF16), pltpu.VMEM(w_key.shape[1:], BF16), pltpu.VMEM(w_value.shape[1:], BF16), pltpu.VMEM(w_out.shape[1:], BF16),
                    pltpu.VMEM((n_tok, rows, head_dim), BF16), pltpu.VMEM((n_tok, rows, head_dim), BF16),
                    pltpu.VMEM((n_tok, pad_heads, head_dim), F32), pltpu.VMEM((n_tok, pad_heads, head_dim), F32),
                    pltpu.VMEM((n_tok, pad_heads, head_dim), F32), pltpu.VMEM((n_tok, pad_heads, head_dim), F32),
                    pltpu.VMEM((n_tok, q_heads * head_dim), BF16),
                    pltpu.SemaphoreType.DMA((4,)), pltpu.SemaphoreType.DMA((n_tok // TOK_STEP,)), pltpu.SemaphoreType.DMA((n_tok // TOK_STEP,)),
                ],
                compiler_params=pltpu.CompilerParams(vmem_limit_bytes=VMEM_BYTES),
            )(lens, x_cur, cos2, sin2, ids[layer], router_t[layer], w_query, w_key, w_value, w_out, k_rows, v_rows)
            d_ff = shared_gate.shape[2]
            x_cur = pl.pallas_call(
                functools.partial(moe_kernel, layer, capacity, ep_size),
                name=f"moe_{layer}",
                out_shape=jax.ShapeDtypeStruct((n_tok, d_model), BF16),
                in_specs=[VMEM] * 3 + [ANY] * 6,
                out_specs=VMEM,
                scratch_shapes=[
                    pltpu.VMEM((ep_size, n_tok, ext), BF16), pltpu.VMEM((ep_size, capacity, d_model), BF16),
                    pltpu.VMEM((ep_size * capacity, d_model), BF16), pltpu.VMEM((ep_size, capacity, d_model), BF16),
                    pltpu.VMEM((ep_size * capacity, d_model), F32), pltpu.VMEM((n_tok, d_model), F32),
                    pltpu.VMEM((RING, d_model, FF_CHUNK), BF16), pltpu.VMEM((RING, d_model, FF_CHUNK), BF16), pltpu.VMEM((RING, FF_CHUNK, d_model), BF16),
                    pltpu.SemaphoreType.DMA((RING, 3)), pltpu.SemaphoreType.DMA((14,)), pltpu.SemaphoreType.DMA((ep_size, 2)),
                    pltpu.SemaphoreType.DMA((ep_size,)), pltpu.SemaphoreType.DMA((ep_size,)),
                ],
                compiler_params=pltpu.CompilerParams(vmem_limit_bytes=VMEM_BYTES, collective_id=layer, has_side_effects=True),
            )(u_ext, resid, meta, shared_gate, shared_up, shared_down, w_gate, w_up, w_down)
        return x_cur

    return jax.shard_map(body, mesh=mesh, in_specs=in_specs, out_specs=row_spec, check_vma=False)
```

```python
import functools
import math
import jax
import jax.numpy as jnp
from jax import lax
from jax.experimental import pallas as pl
from jax.experimental.pallas import tpu as pltpu
from jax.sharding import PartitionSpec as P

RMS_EPS = 1e-6
ROPE_BASE = 10000.0
MESH = pl.DeviceIdType.MESH
BF16 = jnp.bfloat16
F32 = jnp.float32
ANY = pl.BlockSpec(memory_space=pl.ANY)
VMEM = pl.BlockSpec(memory_space=pltpu.VMEM)
SMEM = pl.BlockSpec(memory_space=pltpu.SMEM)
VMEM_BYTES = 66_000_000
META = 128
INFO_LEN = 127
TOK_STEP = 16
FF_CHUNK = 512
LOOKAHEAD = 3
SHARED_CHUNK = 256
SHARED_RING = 4
Q_CHUNK = 256


def rms(vals):
    return vals * lax.rsqrt(jnp.mean(vals * vals, axis=-1, keepdims=True) + RMS_EPS)


def mm(lhs, rhs):
    return jnp.dot(lhs, rhs, preferred_element_type=F32)


def silu(vals):
    return vals * (1.0 / (1.0 + jnp.exp(-vals)))


def attention_kernel(layer, capacity, q_heads, kv_heads, lens, x_ref, info_ref, wr_ref, wq, wk, wv, wo, kc, vc,
                     a_ref, u_ref, meta_ref, wq_b, wk_b, wv_b, wo_b, k_b, v_b, q3, kn3, vn3, o3, attn, w_sem, q_sem, k_sem, v_sem):
    n_tok, d_model = x_ref.shape
    rows = kc.shape[2]
    head_dim = kc.shape[3]
    group = q_heads // kv_heads
    steps = n_tok // TOK_STEP
    q_steps = q_heads * head_dim // Q_CHUNK
    first = lax.axis_index("pool") * n_tok
    scale = head_dim ** -0.5
    k_copy = pltpu.make_async_copy(wk.at[layer], wk_b, w_sem.at[0])
    v_copy = pltpu.make_async_copy(wv.at[layer], wv_b, w_sem.at[1])
    o_copy = pltpu.make_async_copy(wo.at[layer], wo_b, w_sem.at[2])

    def q_copy(step):
        cols = pl.ds(step * Q_CHUNK, Q_CHUNK)
        return pltpu.make_async_copy(wq.at[layer, :, cols], wq_b.at[:, cols], q_sem.at[step])

    def cache_copies(step):
        here = pl.ds(step * TOK_STEP, TOK_STEP)
        there = pl.ds(first + step * TOK_STEP, TOK_STEP)
        return (pltpu.make_async_copy(kc.at[layer, there], k_b.at[here], k_sem.at[step]),
                pltpu.make_async_copy(vc.at[layer, there], v_b.at[here], v_sem.at[step]))

    k_copy.start()
    v_copy.start()
    for step in range(q_steps):
        q_copy(step).start()

    q3[:, q_heads:, :] = jnp.zeros((n_tok, q3.shape[1] - q_heads, head_dim), F32)
    kn3[:, q_heads:, :] = jnp.zeros((n_tok, q3.shape[1] - q_heads, head_dim), F32)
    vn3[:, q_heads:, :] = jnp.zeros((n_tok, q3.shape[1] - q_heads, head_dim), F32)
    x_f = x_ref[...].astype(F32)
    hidden = rms(x_f).astype(BF16)
    lane_d = lax.broadcasted_iota(jnp.int32, (n_tok, head_dim), 1)
    half = head_dim // 2
    inv_freq = jnp.exp(lax.rem(lane_d, half).astype(F32) * (-math.log(ROPE_BASE) / half))
    angle = info_ref[:, INFO_LEN:INFO_LEN + 1].astype(F32) * inv_freq
    cosine = jnp.cos(angle)
    sine = jnp.sin(angle)
    sine = jnp.where(lane_d < half, -sine, sine)

    def rotated(vals):
        return (vals * cosine + pltpu.roll(vals, half, 1) * sine).astype(BF16).astype(F32)

    k_copy.wait()
    key = mm(hidden, wk_b[...])
    v_copy.wait()
    val = mm(hidden, wv_b[...]).astype(BF16).astype(F32)
    for kv in range(kv_heads):
        cols = slice(kv * head_dim, (kv + 1) * head_dim)
        key_rot = rotated(key[:, cols])
        for head in range(kv * group, (kv + 1) * group):
            kn3[:, head, :] = key_rot
            vn3[:, head, :] = val[:, cols]
    started = 0
    for step in range(q_steps):
        q_copy(step).wait()
        upto = (step + 1) * steps // q_steps
        for ready in range(started, upto):
            for copy in cache_copies(ready):
                copy.start()
        started = upto
        query = mm(hidden, wq_b[:, step * Q_CHUNK:(step + 1) * Q_CHUNK])
        for i in range(Q_CHUNK // head_dim):
            q3[:, step * (Q_CHUNK // head_dim) + i, :] = rotated(query[:, i * head_dim:(i + 1) * head_dim])
    o_copy.start()

    pad = q3.shape[1]
    lane = lax.broadcasted_iota(jnp.int32, (pad, rows), 1)
    head_kv = lax.broadcasted_iota(jnp.int32, (pad, rows), 0) // group
    right_kv = lane % kv_heads == head_kv
    position = lane // kv_heads

    def step_body(step, carry):
        for copy in cache_copies(step):
            copy.wait()
        base = step * TOK_STEP
        q_f = q3[pl.ds(base, TOK_STEP)]
        scores = lax.dot_general(q_f.astype(BF16), k_b[pl.ds(base, TOK_STEP)], (((2,), (2,)), ((0,), (0,))), preferred_element_type=F32)
        s_new = jnp.sum(q_f * kn3[pl.ds(base, TOK_STEP)], axis=-1, keepdims=True) * scale
        probs = []
        p_news = []
        for i in range(TOK_STEP):
            valid = right_kv & (position < lens[first + base + i])
            s_i = jnp.where(valid, scores[i] * scale, -jnp.inf)
            peak = jnp.maximum(jnp.max(s_i, axis=-1, keepdims=True), s_new[i])
            e_i = jnp.exp(s_i - peak)
            e_new = jnp.exp(s_new[i] - peak)
            total = jnp.sum(e_i, axis=-1, keepdims=True) + e_new
            probs.append((e_i / total).astype(BF16))
            p_news.append((e_new / total).astype(BF16).astype(F32))
        for i in range(TOK_STEP):
            mixed = mm(probs[i], v_b[base + i])
            o3[base + i] = mixed + p_news[i] * vn3[base + i]
        return carry

    lax.fori_loop(0, steps, step_body, 0)
    for head in range(q_heads):
        attn[:, head * head_dim:(head + 1) * head_dim] = o3[:, head, :].astype(BF16)
    o_copy.wait()
    resid = (x_f + mm(attn[...], wo_b[...])).astype(BF16)
    a_ref[...] = resid
    normed = rms(resid.astype(F32)).astype(BF16)
    u_ref[:, :d_model] = normed

    logits = lax.dot_general(normed.astype(F32), wr_ref[layer], (((1,), (1,)), ((), ())), precision=lax.Precision.HIGHEST, preferred_element_type=F32)
    experts = logits.shape[1]
    lane_e = lax.broadcasted_iota(jnp.int32, (n_tok, META), 1)
    id0 = info_ref[:, 2 * layer:2 * layer + 1]
    id1 = info_ref[:, 2 * layer + 1:2 * layer + 2]
    pick0 = lane_e == id0
    pick1 = lane_e == id1
    l0 = jnp.sum(jnp.where(pick0[:, :experts], logits, 0.0), axis=-1, keepdims=True)
    l1 = jnp.sum(jnp.where(pick1[:, :experts], logits, 0.0), axis=-1, keepdims=True)
    peak = jnp.maximum(l0, l1)
    e0 = jnp.exp(l0 - peak)
    e1 = jnp.exp(l1 - peak)
    member = jnp.where(pick0 | pick1, 1.0, 0.0)
    earlier = jnp.where(lax.broadcasted_iota(jnp.int32, (n_tok, n_tok), 1) < lax.broadcasted_iota(jnp.int32, (n_tok, n_tok), 0), 1.0, 0.0)
    rank = mm(earlier.astype(BF16), member.astype(BF16))
    u_ref[:, d_model:] = jnp.where(member > 0.0, rank, -1.0).astype(BF16)
    slot0 = id0.astype(F32) * capacity + jnp.sum(jnp.where(pick0, rank, 0.0), axis=-1, keepdims=True)
    slot1 = id1.astype(F32) * capacity + jnp.sum(jnp.where(pick1, rank, 0.0), axis=-1, keepdims=True)
    total = e0 + e1
    meta_ref[...] = jnp.where(lane_e == 0, slot0, jnp.where(lane_e == 1, slot1, jnp.where(lane_e == 2, e0 / total, e1 / total)))


def moe_kernel(layer, capacity, ep_size, u_ref, a_ref, meta_ref, sg, su, sd, wg, wu, wd, out_ref,
               gath, back, picked, sent, acc_e, acc_s, g_w, u_w, d_w, g_b, u_b, d_b, e_sem, s_sem, ag_send, ag_recv, ret_send, ret_recv):
    n_tok = a_ref.shape[0]
    d_model = a_ref.shape[1]
    half = n_tok // 2
    e_chunks = wg.shape[3] // FF_CHUNK
    s_chunks = sg.shape[2] // SHARED_CHUNK
    me = lax.axis_index("ep")
    partner = me + 1 - 2 * lax.rem(me, 2)
    right = lax.rem(me + 2, ep_size)
    left = lax.rem(me + ep_size - 2, ep_size)
    far = lax.rem(me + ep_size // 2, ep_size)
    p_right = lax.rem(partner + 2, ep_size)
    p_left = lax.rem(partner + ep_size - 2, ep_size)
    p_far = lax.rem(partner + ep_size // 2, ep_size)
    places = [me, partner, far, p_far, right, p_right, left, p_left]

    def expert_copies(chunk):
        cols = pl.ds(chunk * FF_CHUNK, FF_CHUNK)
        pairs = ((wg.at[layer, 0, :, cols], g_w.at[:, cols]), (wu.at[layer, 0, :, cols], u_w.at[:, cols]), (wd.at[layer, 0, cols], d_w.at[cols]))
        return [pltpu.make_async_copy(src, dst, e_sem.at[chunk, i]) for i, (src, dst) in enumerate(pairs)]

    def shared_copies(chunk, slot):
        cols = pl.ds(chunk * SHARED_CHUNK, SHARED_CHUNK)
        pairs = ((sg.at[layer, :, cols], g_b.at[slot]), (su.at[layer, :, cols], u_b.at[slot]), (sd.at[layer, cols], d_b.at[slot]))
        return [pltpu.make_async_copy(src, dst, s_sem.at[slot, i]) for i, (src, dst) in enumerate(pairs)]

    for chunk in range(LOOKAHEAD):
        for copy in expert_copies(chunk):
            copy.start()

    barrier = pltpu.get_barrier_semaphore()
    for other in range(1, ep_size):
        pl.semaphore_signal(barrier, inc=1, device_id={"ep": lax.rem(me + other, ep_size)}, device_id_type=MESH)
    gath[me] = u_ref[...]
    pl.semaphore_wait(barrier, ep_size - 1)

    def piece(src, part):
        return gath.at[src, pl.ds(part * half, half)]

    def arrived(src, part):
        pltpu.make_async_remote_copy(src_ref=piece(src, part), dst_ref=piece(src, part), send_sem=ag_send.at[0], recv_sem=ag_recv.at[src, part],
                                     device_id={"ep": partner}, device_id_type=MESH).wait_recv()

    sends = []

    def send(src, part, target, from_input=False):
        ref = u_ref.at[pl.ds(part * half, half)] if from_input else piece(src, part)
        copy = pltpu.make_async_remote_copy(src_ref=ref, dst_ref=piece(src, part), send_sem=ag_send.at[len(sends)], recv_sem=ag_recv.at[src, part],
                                            device_id={"ep": target}, device_id_type=MESH)
        copy.start()
        sends.append(copy)

    send(me, 0, partner, True)
    send(me, 1, partner, True)
    send(me, 0, right, True)
    send(me, 1, left, True)
    send(me, 1, right, True)
    send(me, 0, left, True)

    acc_s[...] = jnp.zeros_like(acc_s)
    acc_e[...] = jnp.zeros_like(acc_e)
    lane = lax.broadcasted_iota(jnp.int32, (n_tok, META), 1)

    def pick(src, codes, values, place):
        rank = jnp.sum(jnp.where(lane == me, codes.astype(F32), 0.0), axis=-1, keepdims=True)
        choose = jnp.where(lane.astype(F32) == rank, 1.0, 0.0).astype(BF16)
        rows = lax.dot_general(choose, values, (((0,), (0,)), ((), ())), preferred_element_type=F32)
        picked[pl.ds(place * capacity, capacity)] = rows[:capacity].astype(BF16)

    def pick_places(first, last):
        for place in range(first, last):
            src = places[place]
            if place == 0:
                pick(src, u_ref[:, d_model:], u_ref[:, :d_model], place)
            else:
                pick(src, gath[src, :, d_model:], gath[src, :, :d_model], place)

    def expert_rows(first, last, chunk):
        rows = pl.ds(first * capacity, (last - first) * capacity)
        cols = pl.ds(pl.multiple_of(chunk * FF_CHUNK, FF_CHUNK), FF_CHUNK)
        x_rows = picked[rows]
        mid = (silu(mm(x_rows, g_w[:, cols])) * mm(x_rows, u_w[:, cols])).astype(BF16)
        acc_e[rows] += mm(mid, d_w[cols])

    def return_copy(place):
        target = places[place]
        return pltpu.make_async_remote_copy(src_ref=sent.at[place], dst_ref=back.at[me], send_sem=ret_send.at[place], recv_sem=ret_recv.at[me],
                                            device_id={"ep": target}, device_id_type=MESH)

    def give_back(first, last):
        for place in range(first, last):
            sent[place] = acc_e[pl.ds(place * capacity, capacity)].astype(BF16)
        for place in range(max(first, 1), last):
            return_copy(place).start()

    def own_step(chunk, carry):
        for copy in expert_copies(chunk):
            copy.wait()

        @pl.when(chunk + LOOKAHEAD < e_chunks)
        def _():
            for copy in expert_copies(chunk + LOOKAHEAD):
                copy.start()

        expert_rows(0, 2, chunk)
        return carry

    for part in (0, 1):
        arrived(partner, part)
    pick_places(0, 2)
    lax.fori_loop(0, 2, own_step, 0)
    arrived(left, 0)
    send(left, 0, right)
    arrived(right, 1)
    send(right, 1, left)
    send(left, 0, partner)
    send(right, 1, partner)
    lax.fori_loop(2, 4, own_step, 0)
    for src, part in ((left, 1), (right, 0)):
        arrived(src, part)
        send(src, part, partner)
    lax.fori_loop(4, 6, own_step, 0)
    for slot in range(SHARED_RING):
        for copy in shared_copies(slot, slot):
            copy.start()
    for src, part in ((far, 0), (far, 1)):
        arrived(src, part)
        send(src, part, partner)
    lax.fori_loop(6, e_chunks, own_step, 0)
    give_back(0, 2)
    for src in (p_right, p_left, p_far):
        for part in (0, 1):
            arrived(src, part)

    def full_pass(first, last):
        pick_places(first, last)

        def step(chunk, carry):
            expert_rows(first, last, chunk)
            return carry

        lax.fori_loop(0, e_chunks, step, 0)
        give_back(first, last)

    full_pass(2, 4)
    full_pass(4, 8)

    def shared_step(chunk, carry):
        slot = lax.rem(chunk, SHARED_RING)
        for copy in shared_copies(chunk, slot):
            copy.wait()
        rows = u_ref[:, :d_model]
        mid = (silu(mm(rows, g_b[slot])) * mm(rows, u_b[slot])).astype(BF16)
        acc_s[...] += mm(mid, d_b[slot])

        @pl.when(chunk + SHARED_RING < s_chunks)
        def _():
            for copy in shared_copies(chunk + SHARED_RING, slot):
                copy.start()

        return carry

    lax.fori_loop(0, s_chunks, shared_step, 0)
    back[me] = sent[0]
    for copy in sends:
        copy.wait_send()
    for place in range(1, ep_size):
        return_copy(place).wait_send()
        src = places[place]
        pltpu.make_async_remote_copy(src_ref=back.at[src], dst_ref=back.at[src], send_sem=ret_send.at[place], recv_sem=ret_recv.at[src],
                                     device_id={"ep": src}, device_id_type=MESH).wait_recv()

    slot_lane = lax.broadcasted_iota(jnp.int32, (n_tok, ep_size * capacity), 1).astype(F32)
    table = back[...].reshape(ep_size * capacity, d_model)
    y0 = mm(jnp.where(slot_lane == meta_ref[:, 0:1], 1.0, 0.0).astype(BF16), table)
    y1 = mm(jnp.where(slot_lane == meta_ref[:, 1:2], 1.0, 0.0).astype(BF16), table)
    routed = meta_ref[:, 2:3] * y0 + meta_ref[:, 3:4] * y1
    out_ref[...] = (a_ref[...].astype(F32) + routed + acc_s[...].astype(BF16).astype(F32)).astype(BF16)


def solution(mesh):
    ep_size = mesh.shape["ep"]
    row_spec = P(("dp", "ep", "pool"), None)
    cache_spec = P(None, ("dp", "ep"), None, None, None)
    expert_spec = P(None, "ep", None, None)
    in_specs = (row_spec, cache_spec, cache_spec, P(("dp", "ep")), P(), P(), P(), P(), P(), P(None, ("dp", "ep"), None), expert_spec, expert_spec, expert_spec, P(), P(), P())

    def body(x_loc, k_cache, v_cache, cache_len, w_query, w_key, w_value, w_out, w_router, expert_ids, w_gate, w_up, w_down, shared_gate, shared_up, shared_down):
        n_tok, d_model = x_loc.shape
        n_layers, all_tok, ctx, kv_heads, head_dim = k_cache.shape
        q_heads = w_query.shape[2] // head_dim
        top_k = expert_ids.shape[2]
        capacity = 3 * n_tok * top_k // ep_size
        rows = ctx * kv_heads
        pad_heads = -(-q_heads // 8) * 8
        first = lax.axis_index("pool") * n_tok
        lens = lax.dynamic_slice_in_dim(cache_len, first, n_tok, 0)
        ids = lax.dynamic_slice_in_dim(expert_ids, first, n_tok, 1)
        lane = lax.broadcasted_iota(jnp.int32, (n_tok, META), 1)
        info = jnp.where(lane == INFO_LEN, lens[:, None], 0)
        for layer in range(n_layers):
            for choice in range(top_k):
                info = jnp.where(lane == layer * top_k + choice, ids[layer, :, choice][:, None], info)
        router_t = jnp.swapaxes(w_router, 1, 2)
        k_rows = k_cache.reshape(n_layers, all_tok, rows, head_dim)
        v_rows = v_cache.reshape(n_layers, all_tok, rows, head_dim)
        ext = d_model + META
        x_cur = x_loc
        for layer in range(n_layers):
            resid, u_ext, meta = pl.pallas_call(
                functools.partial(attention_kernel, layer, capacity, q_heads, kv_heads),
                name=f"attention_{layer}",
                out_shape=(jax.ShapeDtypeStruct((n_tok, d_model), BF16), jax.ShapeDtypeStruct((n_tok, ext), BF16), jax.ShapeDtypeStruct((n_tok, META), F32)),
                in_specs=[SMEM] + [VMEM] * 3 + [ANY] * 6,
                out_specs=(VMEM, VMEM, VMEM),
                scratch_shapes=[
                    pltpu.VMEM(w_query.shape[1:], BF16), pltpu.VMEM(w_key.shape[1:], BF16), pltpu.VMEM(w_value.shape[1:], BF16), pltpu.VMEM(w_out.shape[1:], BF16),
                    pltpu.VMEM((n_tok, rows, head_dim), BF16), pltpu.VMEM((n_tok, rows, head_dim), BF16),
                    pltpu.VMEM((n_tok, pad_heads, head_dim), F32), pltpu.VMEM((n_tok, pad_heads, head_dim), F32),
                    pltpu.VMEM((n_tok, pad_heads, head_dim), F32), pltpu.VMEM((n_tok, pad_heads, head_dim), F32),
                    pltpu.VMEM((n_tok, q_heads * head_dim), BF16),
                    pltpu.SemaphoreType.DMA((3,)), pltpu.SemaphoreType.DMA((q_heads * head_dim // Q_CHUNK,)), pltpu.SemaphoreType.DMA((n_tok // TOK_STEP,)), pltpu.SemaphoreType.DMA((n_tok // TOK_STEP,)),
                ],
                compiler_params=pltpu.CompilerParams(vmem_limit_bytes=VMEM_BYTES),
            )(cache_len, x_cur, info, router_t, w_query, w_key, w_value, w_out, k_rows, v_rows)
            x_cur = pl.pallas_call(
                functools.partial(moe_kernel, layer, capacity, ep_size),
                name=f"moe_{layer}",
                out_shape=jax.ShapeDtypeStruct((n_tok, d_model), BF16),
                in_specs=[VMEM] * 3 + [ANY] * 6,
                out_specs=VMEM,
                scratch_shapes=[
                    pltpu.VMEM((ep_size, n_tok, ext), BF16), pltpu.VMEM((ep_size, capacity, d_model), BF16),
                    pltpu.VMEM((ep_size * capacity, d_model), BF16), pltpu.VMEM((ep_size, capacity, d_model), BF16),
                    pltpu.VMEM((ep_size * capacity, d_model), F32), pltpu.VMEM((n_tok, d_model), F32),
                    pltpu.VMEM(w_gate.shape[2:], BF16), pltpu.VMEM(w_up.shape[2:], BF16), pltpu.VMEM(w_down.shape[2:], BF16),
                    pltpu.VMEM((SHARED_RING, d_model, SHARED_CHUNK), BF16), pltpu.VMEM((SHARED_RING, d_model, SHARED_CHUNK), BF16), pltpu.VMEM((SHARED_RING, SHARED_CHUNK, d_model), BF16),
                    pltpu.SemaphoreType.DMA((w_gate.shape[3] // FF_CHUNK, 3)), pltpu.SemaphoreType.DMA((SHARED_RING, 3)), pltpu.SemaphoreType.DMA((14,)), pltpu.SemaphoreType.DMA((ep_size, 2)),
                    pltpu.SemaphoreType.DMA((ep_size,)), pltpu.SemaphoreType.DMA((ep_size,)),
                ],
                compiler_params=pltpu.CompilerParams(vmem_limit_bytes=VMEM_BYTES, collective_id=layer, has_side_effects=True),
            )(u_ext, resid, meta, shared_gate, shared_up, shared_down, w_gate, w_up, w_down)
        return x_cur

    return jax.shard_map(body, mesh=mesh, in_specs=in_specs, out_specs=row_spec, check_vma=False)
```

```python
import functools
import math
import jax
import jax.numpy as jnp
from jax import lax
from jax.experimental import pallas as pl
from jax.experimental.pallas import tpu as pltpu
from jax.sharding import PartitionSpec as P

RMS_EPS = 1e-6
ROPE_BASE = 10000.0
MESH = pl.DeviceIdType.MESH
BF16 = jnp.bfloat16
F32 = jnp.float32
ANY = pl.BlockSpec(memory_space=pl.ANY)
VMEM = pl.BlockSpec(memory_space=pltpu.VMEM)
SMEM = pl.BlockSpec(memory_space=pltpu.SMEM)
VMEM_BYTES = 66_000_000
META = 128
INFO_LEN = 127
TOK_STEP = 16
FF_CHUNK = 512
LOOKAHEAD = 3
PASS_CHUNK = 2048
SHARED_CHUNK = 512
SHARED_RING = 2
Q_CHUNK = 512
CHIP_CORES = 2
ROW_TILE = 128


def rms(vals):
    return vals * lax.rsqrt(jnp.mean(vals * vals, axis=-1, keepdims=True) + RMS_EPS)


def mm(lhs, rhs):
    return jnp.dot(lhs, rhs, preferred_element_type=F32)


def silu(vals):
    return vals * (1.0 / (1.0 + jnp.exp(-vals)))


def attention_kernel(layer, capacity, q_heads, kv_heads, lens, x_ref, info_ref, wr_ref, wq, wk, wv, wo, kc, vc,
                     a_ref, u_ref, meta_ref, wq_b, wk_b, wv_b, wo_b, k_b, v_b, q3, kn3, vn3, o3, attn, w_sem, q_sem, k_sem, v_sem):
    n_tok, d_model = x_ref.shape
    rows = kc.shape[2]
    head_dim = kc.shape[3]
    group = q_heads // kv_heads
    steps = n_tok // TOK_STEP
    q_steps = q_heads * head_dim // Q_CHUNK
    first = lax.axis_index("pool") * n_tok
    scale = head_dim ** -0.5
    k_copy = pltpu.make_async_copy(wk.at[layer], wk_b, w_sem.at[0])
    v_copy = pltpu.make_async_copy(wv.at[layer], wv_b, w_sem.at[1])
    o_copy = pltpu.make_async_copy(wo.at[layer], wo_b, w_sem.at[2])

    def q_copy(step):
        cols = pl.ds(step * Q_CHUNK, Q_CHUNK)
        return pltpu.make_async_copy(wq.at[layer, :, cols], wq_b.at[:, cols], q_sem.at[step])

    def cache_copies(step):
        here = pl.ds(step * TOK_STEP, TOK_STEP)
        there = pl.ds(first + step * TOK_STEP, TOK_STEP)
        return (pltpu.make_async_copy(kc.at[layer, there], k_b.at[here], k_sem.at[step]),
                pltpu.make_async_copy(vc.at[layer, there], v_b.at[here], v_sem.at[step]))

    def start_cache(step):
        for copy in cache_copies(step):
            copy.start()

    k_copy.start()
    v_copy.start()
    q_copy(0).start()

    q3[:, q_heads:, :] = jnp.zeros((n_tok, q3.shape[1] - q_heads, head_dim), F32)
    kn3[:, q_heads:, :] = jnp.zeros((n_tok, q3.shape[1] - q_heads, head_dim), F32)
    vn3[:, q_heads:, :] = jnp.zeros((n_tok, q3.shape[1] - q_heads, head_dim), F32)
    x_f = x_ref[...].astype(F32)
    hidden = rms(x_f).astype(BF16)
    lane_d = lax.broadcasted_iota(jnp.int32, (n_tok, head_dim), 1)
    half = head_dim // 2
    inv_freq = jnp.exp(lax.rem(lane_d, half).astype(F32) * (-math.log(ROPE_BASE) / half))
    angle = info_ref[:, INFO_LEN:INFO_LEN + 1].astype(F32) * inv_freq
    cosine = jnp.cos(angle)
    sine = jnp.sin(angle)
    sine = jnp.where(lane_d < half, -sine, sine)

    def rotated(vals):
        return (vals * cosine + pltpu.roll(vals, half, 1) * sine).astype(BF16).astype(F32)

    k_copy.wait()
    q_copy(1).start()
    key = mm(hidden, wk_b[...])
    v_copy.wait()
    q_copy(2).start()
    val = mm(hidden, wv_b[...]).astype(BF16).astype(F32)
    for kv in range(kv_heads):
        cols = slice(kv * head_dim, (kv + 1) * head_dim)
        key_rot = rotated(key[:, cols])
        for head in range(kv * group, (kv + 1) * group):
            kn3[:, head, :] = key_rot
            vn3[:, head, :] = val[:, cols]
    for step in range(q_steps):
        q_copy(step).wait()
        start_cache(step)
        query = mm(hidden, wq_b[:, step * Q_CHUNK:(step + 1) * Q_CHUNK])
        for i in range(Q_CHUNK // head_dim):
            q3[:, step * (Q_CHUNK // head_dim) + i, :] = rotated(query[:, i * head_dim:(i + 1) * head_dim])
    for step in range(q_steps, steps):
        start_cache(step)
    o_copy.start()

    pad = q3.shape[1]
    lane = lax.broadcasted_iota(jnp.int32, (pad, rows), 1)
    head_kv = lax.broadcasted_iota(jnp.int32, (pad, rows), 0) // group
    right_kv = lane % kv_heads == head_kv
    position = lane // kv_heads

    def step_body(step, carry):
        for copy in cache_copies(step):
            copy.wait()
        base = step * TOK_STEP
        q_f = q3[pl.ds(base, TOK_STEP)]
        scores = lax.dot_general(q_f.astype(BF16), k_b[pl.ds(base, TOK_STEP)], (((2,), (2,)), ((0,), (0,))), preferred_element_type=F32)
        s_new = jnp.sum(q_f * kn3[pl.ds(base, TOK_STEP)], axis=-1, keepdims=True) * scale
        probs = []
        p_news = []
        for i in range(TOK_STEP):
            valid = right_kv & (position < lens[first + base + i])
            s_i = jnp.where(valid, scores[i] * scale, -jnp.inf)
            peak = jnp.maximum(jnp.max(s_i, axis=-1, keepdims=True), s_new[i])
            e_i = jnp.exp(s_i - peak)
            e_new = jnp.exp(s_new[i] - peak)
            total = jnp.sum(e_i, axis=-1, keepdims=True) + e_new
            probs.append((e_i / total).astype(BF16))
            p_news.append((e_new / total).astype(BF16).astype(F32))
        for i in range(TOK_STEP):
            mixed = mm(probs[i], v_b[base + i])
            o3[base + i] = mixed + p_news[i] * vn3[base + i]
        return carry

    lax.fori_loop(0, steps, step_body, 0)
    for head in range(q_heads):
        attn[:, head * head_dim:(head + 1) * head_dim] = o3[:, head, :].astype(BF16)
    o_copy.wait()
    resid = (x_f + mm(attn[...], wo_b[...])).astype(BF16)
    a_ref[...] = resid
    normed = rms(resid.astype(F32)).astype(BF16)
    u_ref[:, :d_model] = normed

    logits = lax.dot_general(normed.astype(F32), wr_ref[layer], (((1,), (1,)), ((), ())), precision=lax.Precision.HIGHEST, preferred_element_type=F32)
    experts = logits.shape[1]
    lane_e = lax.broadcasted_iota(jnp.int32, (n_tok, META), 1)
    id0 = info_ref[:, 2 * layer:2 * layer + 1]
    id1 = info_ref[:, 2 * layer + 1:2 * layer + 2]
    pick0 = lane_e == id0
    pick1 = lane_e == id1
    l0 = jnp.sum(jnp.where(pick0[:, :experts], logits, 0.0), axis=-1, keepdims=True)
    l1 = jnp.sum(jnp.where(pick1[:, :experts], logits, 0.0), axis=-1, keepdims=True)
    peak = jnp.maximum(l0, l1)
    e0 = jnp.exp(l0 - peak)
    e1 = jnp.exp(l1 - peak)
    member = jnp.where(pick0 | pick1, 1.0, 0.0)
    earlier = jnp.where(lax.broadcasted_iota(jnp.int32, (n_tok, n_tok), 1) < lax.broadcasted_iota(jnp.int32, (n_tok, n_tok), 0), 1.0, 0.0)
    rank = mm(earlier.astype(BF16), member.astype(BF16))
    u_ref[:, d_model:] = jnp.where(member > 0.0, rank, -1.0).astype(BF16)
    slot0 = id0.astype(F32) * capacity + jnp.sum(jnp.where(pick0, rank, 0.0), axis=-1, keepdims=True)
    slot1 = id1.astype(F32) * capacity + jnp.sum(jnp.where(pick1, rank, 0.0), axis=-1, keepdims=True)
    total = e0 + e1
    meta_ref[...] = jnp.where(lane_e == 0, slot0, jnp.where(lane_e == 1, slot1, jnp.where(lane_e == 2, e0 / total, e1 / total)))


def row_blocks(capacity, blocks=((0, 2), (2, 4), (4, 8))):
    sizes = [-(-(hi - lo) * capacity // ROW_TILE) * ROW_TILE if (hi - lo) * capacity < ROW_TILE else (hi - lo) * capacity for lo, hi in blocks]
    return [sum(sizes[:i]) for i in range(len(sizes))], sizes


def moe_kernel(layer, capacity, ep_size, u_ref, a_ref, meta_ref, sg, su, sd, wg, wu, wd, out_ref,
               gath, back, picked, sent, acc_e, acc_s, pair, other_s, g_w, u_w, d_w, g_b, u_b, d_b, e_sem, s_sem, ag_send, ag_recv, ret_send, ret_recv, sum_send, sum_recv):
    n_tok = a_ref.shape[0]
    d_model = a_ref.shape[1]
    half = n_tok // 2
    e_chunks = wg.shape[3] // FF_CHUNK
    s_chunks = sg.shape[2] // (SHARED_CHUNK * CHIP_CORES)
    me = lax.axis_index("ep")
    partner = me + 1 - 2 * lax.rem(me, 2)
    right = lax.rem(me + 2, ep_size)
    left = lax.rem(me + ep_size - 2, ep_size)
    far = lax.rem(me + ep_size // 2, ep_size)
    p_right = lax.rem(partner + 2, ep_size)
    p_left = lax.rem(partner + ep_size - 2, ep_size)
    p_far = lax.rem(partner + ep_size // 2, ep_size)
    places = [me, partner, far, p_far, right, p_right, left, p_left]
    blocks = [(0, 2), (2, 4), (4, 8)]
    starts, sizes = row_blocks(capacity, blocks)
    row_of = {place: starts[i] + (place - lo) * capacity for i, (lo, hi) in enumerate(blocks) for place in range(lo, hi)}

    def expert_copies(chunk):
        cols = pl.ds(chunk * FF_CHUNK, FF_CHUNK)
        pairs = ((wg.at[layer, 0, :, cols], g_w.at[:, cols]), (wu.at[layer, 0, :, cols], u_w.at[:, cols]), (wd.at[layer, 0, cols], d_w.at[cols]))
        return [pltpu.make_async_copy(src, dst, e_sem.at[chunk, i]) for i, (src, dst) in enumerate(pairs)]

    s_first = lax.rem(me, CHIP_CORES) * s_chunks

    def shared_copies(chunk, slot):
        cols = pl.ds((s_first + chunk) * SHARED_CHUNK, SHARED_CHUNK)
        pairs = ((sg.at[layer, :, cols], g_b.at[slot]), (su.at[layer, :, cols], u_b.at[slot]), (sd.at[layer, cols], d_b.at[slot]))
        return [pltpu.make_async_copy(src, dst, s_sem.at[slot, i]) for i, (src, dst) in enumerate(pairs)]

    for chunk in range(LOOKAHEAD):
        for copy in expert_copies(chunk):
            copy.start()

    barrier = pltpu.get_barrier_semaphore()
    for other in range(1, ep_size):
        pl.semaphore_signal(barrier, inc=1, device_id={"ep": lax.rem(me + other, ep_size)}, device_id_type=MESH)
    gath[me] = u_ref[...]
    pl.semaphore_wait(barrier, ep_size - 1)

    def piece(src, part):
        return gath.at[src, pl.ds(part * half, half)]

    def arrived(src, part):
        pltpu.make_async_remote_copy(src_ref=piece(src, part), dst_ref=piece(src, part), send_sem=ag_send.at[0], recv_sem=ag_recv.at[src, part],
                                     device_id={"ep": partner}, device_id_type=MESH).wait_recv()

    sends = []

    def send(src, part, target, from_input=False):
        ref = u_ref.at[pl.ds(part * half, half)] if from_input else piece(src, part)
        copy = pltpu.make_async_remote_copy(src_ref=ref, dst_ref=piece(src, part), send_sem=ag_send.at[len(sends)], recv_sem=ag_recv.at[src, part],
                                            device_id={"ep": target}, device_id_type=MESH)
        copy.start()
        sends.append(copy)

    send(me, 0, partner, True)
    send(me, 1, partner, True)
    send(me, 0, right, True)
    send(me, 1, left, True)
    send(me, 1, right, True)
    send(me, 0, left, True)

    acc_s[...] = jnp.zeros_like(acc_s)
    acc_e[...] = jnp.zeros_like(acc_e)
    picked[...] = jnp.zeros_like(picked)
    lane = lax.broadcasted_iota(jnp.int32, (n_tok, META), 1)

    def pick(src, codes, values, place):
        rank = jnp.sum(jnp.where(lane == me, codes.astype(F32), 0.0), axis=-1, keepdims=True)
        choose = jnp.where(lane.astype(F32) == rank, 1.0, 0.0).astype(BF16)
        rows = lax.dot_general(choose, values, (((0,), (0,)), ((), ())), preferred_element_type=F32)
        picked[pl.ds(row_of[place], capacity)] = rows[:capacity].astype(BF16)

    def pick_places(first, last):
        for place in range(first, last):
            src = places[place]
            if place == 0:
                pick(src, u_ref[:, d_model:], u_ref[:, :d_model], place)
            else:
                pick(src, gath[src, :, d_model:], gath[src, :, :d_model], place)

    def expert_rows(block, chunk, width):
        rows = pl.ds(starts[block], sizes[block])
        cols = pl.ds(pl.multiple_of(chunk * width, width), width)
        x_rows = picked[rows]
        mid = (silu(mm(x_rows, g_w[:, cols])) * mm(x_rows, u_w[:, cols])).astype(BF16)
        acc_e[rows] += mm(mid, d_w[cols])

    def return_copy(place):
        target = places[place]
        return pltpu.make_async_remote_copy(src_ref=sent.at[place], dst_ref=back.at[me], send_sem=ret_send.at[place], recv_sem=ret_recv.at[me],
                                            device_id={"ep": target}, device_id_type=MESH)

    def give_back(first, last):
        for place in range(first, last):
            sent[place] = acc_e[pl.ds(row_of[place], capacity)].astype(BF16)
        for place in range(max(first, 1), last):
            return_copy(place).start()

    def own_step(chunk, carry):
        for copy in expert_copies(chunk):
            copy.wait()

        @pl.when(chunk + LOOKAHEAD < e_chunks)
        def _():
            for copy in expert_copies(chunk + LOOKAHEAD):
                copy.start()

        expert_rows(0, chunk, FF_CHUNK)
        return carry

    for part in (0, 1):
        arrived(partner, part)
    pick_places(0, 2)
    lax.fori_loop(0, 2, own_step, 0)
    arrived(left, 0)
    send(left, 0, right)
    arrived(right, 1)
    send(right, 1, left)
    send(left, 0, partner)
    send(right, 1, partner)
    lax.fori_loop(2, 4, own_step, 0)
    for src, part in ((left, 1), (right, 0)):
        arrived(src, part)
        send(src, part, partner)
    lax.fori_loop(4, 6, own_step, 0)
    for slot in range(SHARED_RING):
        for copy in shared_copies(slot, slot):
            copy.start()
    for src, part in ((far, 0), (far, 1)):
        arrived(src, part)
        send(src, part, partner)
    lax.fori_loop(6, e_chunks, own_step, 0)
    give_back(0, 2)
    for src in (p_right, p_left, p_far):
        for part in (0, 1):
            arrived(src, part)

    def full_pass(block):
        first, last = blocks[block]
        pick_places(first, last)

        def step(chunk, carry):
            expert_rows(block, chunk, PASS_CHUNK)
            return carry

        lax.fori_loop(0, wg.shape[3] // PASS_CHUNK, step, 0)
        give_back(first, last)

    full_pass(1)
    full_pass(2)
    pair[pl.ds(0, n_tok)] = u_ref[:, :d_model]
    pair[pl.ds(n_tok, n_tok)] = gath[partner, :, :d_model]

    def shared_step(chunk, carry):
        slot = lax.rem(chunk, SHARED_RING)
        for copy in shared_copies(chunk, slot):
            copy.wait()
        rows = pair[...]
        mid = (silu(mm(rows, g_b[slot])) * mm(rows, u_b[slot])).astype(BF16)
        acc_s[...] += mm(mid, d_b[slot])

        @pl.when(chunk + SHARED_RING < s_chunks)
        def _():
            for copy in shared_copies(chunk + SHARED_RING, slot):
                copy.start()

        return carry

    lax.fori_loop(0, s_chunks, shared_step, 0)
    sum_copy = pltpu.make_async_remote_copy(src_ref=acc_s.at[pl.ds(n_tok, n_tok)], dst_ref=other_s, send_sem=sum_send, recv_sem=sum_recv,
                                            device_id={"ep": partner}, device_id_type=MESH)
    sum_copy.start()
    back[me] = sent[0]
    for copy in sends:
        copy.wait_send()
    for place in range(1, ep_size):
        return_copy(place).wait_send()
        src = places[place]
        pltpu.make_async_remote_copy(src_ref=back.at[src], dst_ref=back.at[src], send_sem=ret_send.at[place], recv_sem=ret_recv.at[src],
                                     device_id={"ep": src}, device_id_type=MESH).wait_recv()

    slot_lane = lax.broadcasted_iota(jnp.int32, (n_tok, ep_size * capacity), 1).astype(F32)
    table = back[...].reshape(ep_size * capacity, d_model)
    choose = jnp.concatenate([jnp.where(slot_lane == meta_ref[:, 0:1], 1.0, 0.0), jnp.where(slot_lane == meta_ref[:, 1:2], 1.0, 0.0)], axis=0).astype(BF16)
    y_pair = mm(choose, table)
    routed = meta_ref[:, 2:3] * y_pair[:n_tok] + meta_ref[:, 3:4] * y_pair[n_tok:]
    sum_copy.wait()
    shared_out = (acc_s[pl.ds(0, n_tok)] + other_s[...]).astype(BF16).astype(F32)
    out_ref[...] = (a_ref[...].astype(F32) + routed + shared_out).astype(BF16)


def solution(mesh):
    ep_size = mesh.shape["ep"]
    row_spec = P(("dp", "ep", "pool"), None)
    cache_spec = P(None, ("dp", "ep"), None, None, None)
    expert_spec = P(None, "ep", None, None)
    in_specs = (row_spec, cache_spec, cache_spec, P(("dp", "ep")), P(), P(), P(), P(), P(), P(None, ("dp", "ep"), None), expert_spec, expert_spec, expert_spec, P(), P(), P())

    def body(x_loc, k_cache, v_cache, cache_len, w_query, w_key, w_value, w_out, w_router, expert_ids, w_gate, w_up, w_down, shared_gate, shared_up, shared_down):
        n_tok, d_model = x_loc.shape
        n_layers, all_tok, ctx, kv_heads, head_dim = k_cache.shape
        q_heads = w_query.shape[2] // head_dim
        top_k = expert_ids.shape[2]
        capacity = 3 * n_tok * top_k // ep_size
        rows = ctx * kv_heads
        pad_heads = -(-q_heads // 8) * 8
        first = lax.axis_index("pool") * n_tok
        lens = lax.dynamic_slice_in_dim(cache_len, first, n_tok, 0)
        ids = lax.dynamic_slice_in_dim(expert_ids, first, n_tok, 1)
        lane = lax.broadcasted_iota(jnp.int32, (n_tok, META), 1)
        info = jnp.where(lane == INFO_LEN, lens[:, None], 0)
        for layer in range(n_layers):
            for choice in range(top_k):
                info = jnp.where(lane == layer * top_k + choice, ids[layer, :, choice][:, None], info)
        router_t = jnp.swapaxes(w_router, 1, 2)
        k_rows = k_cache.reshape(n_layers, all_tok, rows, head_dim)
        v_rows = v_cache.reshape(n_layers, all_tok, rows, head_dim)
        ext = d_model + META
        n_rows = sum(row_blocks(capacity)[1])
        x_cur = x_loc
        for layer in range(n_layers):
            resid, u_ext, meta = pl.pallas_call(
                functools.partial(attention_kernel, layer, capacity, q_heads, kv_heads),
                name=f"attention_{layer}",
                out_shape=(jax.ShapeDtypeStruct((n_tok, d_model), BF16), jax.ShapeDtypeStruct((n_tok, ext), BF16), jax.ShapeDtypeStruct((n_tok, META), F32)),
                in_specs=[SMEM] + [VMEM] * 3 + [ANY] * 6,
                out_specs=(VMEM, VMEM, VMEM),
                scratch_shapes=[
                    pltpu.VMEM(w_query.shape[1:], BF16), pltpu.VMEM(w_key.shape[1:], BF16), pltpu.VMEM(w_value.shape[1:], BF16), pltpu.VMEM(w_out.shape[1:], BF16),
                    pltpu.VMEM((n_tok, rows, head_dim), BF16), pltpu.VMEM((n_tok, rows, head_dim), BF16),
                    pltpu.VMEM((n_tok, pad_heads, head_dim), F32), pltpu.VMEM((n_tok, pad_heads, head_dim), F32),
                    pltpu.VMEM((n_tok, pad_heads, head_dim), F32), pltpu.VMEM((n_tok, pad_heads, head_dim), F32),
                    pltpu.VMEM((n_tok, q_heads * head_dim), BF16),
                    pltpu.SemaphoreType.DMA((3,)), pltpu.SemaphoreType.DMA((q_heads * head_dim // Q_CHUNK,)), pltpu.SemaphoreType.DMA((n_tok // TOK_STEP,)), pltpu.SemaphoreType.DMA((n_tok // TOK_STEP,)),
                ],
                compiler_params=pltpu.CompilerParams(vmem_limit_bytes=VMEM_BYTES),
            )(cache_len, x_cur, info, router_t, w_query, w_key, w_value, w_out, k_rows, v_rows)
            x_cur = pl.pallas_call(
                functools.partial(moe_kernel, layer, capacity, ep_size),
                name=f"moe_{layer}",
                out_shape=jax.ShapeDtypeStruct((n_tok, d_model), BF16),
                in_specs=[VMEM] * 3 + [ANY] * 6,
                out_specs=VMEM,
                scratch_shapes=[
                    pltpu.VMEM((ep_size, n_tok, ext), BF16), pltpu.VMEM((ep_size, capacity, d_model), BF16),
                    pltpu.VMEM((n_rows, d_model), BF16), pltpu.VMEM((ep_size, capacity, d_model), BF16),
                    pltpu.VMEM((n_rows, d_model), F32), pltpu.VMEM((CHIP_CORES * n_tok, d_model), F32),
                    pltpu.VMEM((CHIP_CORES * n_tok, d_model), BF16), pltpu.VMEM((n_tok, d_model), F32),
                    pltpu.VMEM(w_gate.shape[2:], BF16), pltpu.VMEM(w_up.shape[2:], BF16), pltpu.VMEM(w_down.shape[2:], BF16),
                    pltpu.VMEM((SHARED_RING, d_model, SHARED_CHUNK), BF16), pltpu.VMEM((SHARED_RING, d_model, SHARED_CHUNK), BF16), pltpu.VMEM((SHARED_RING, SHARED_CHUNK, d_model), BF16),
                    pltpu.SemaphoreType.DMA((w_gate.shape[3] // FF_CHUNK, 3)), pltpu.SemaphoreType.DMA((SHARED_RING, 3)), pltpu.SemaphoreType.DMA((14,)), pltpu.SemaphoreType.DMA((ep_size, 2)),
                    pltpu.SemaphoreType.DMA((ep_size,)), pltpu.SemaphoreType.DMA((ep_size,)), pltpu.SemaphoreType.DMA, pltpu.SemaphoreType.DMA,
                ],
                compiler_params=pltpu.CompilerParams(vmem_limit_bytes=VMEM_BYTES, collective_id=layer, has_side_effects=True),
            )(u_ext, resid, meta, shared_gate, shared_up, shared_down, w_gate, w_up, w_down)
        return x_cur

    return jax.shard_map(body, mesh=mesh, in_specs=in_specs, out_specs=row_spec, check_vma=False)
```

```python
import functools
import math
import jax
import jax.numpy as jnp
from jax import lax
from jax.experimental import pallas as pl
from jax.experimental.pallas import tpu as pltpu
from jax.sharding import PartitionSpec as P

RMS_EPS = 1e-6
ROPE_BASE = 10000.0
MESH = pl.DeviceIdType.MESH
BF16 = jnp.bfloat16
F32 = jnp.float32
ANY = pl.BlockSpec(memory_space=pl.ANY)
VMEM = pl.BlockSpec(memory_space=pltpu.VMEM)
SMEM = pl.BlockSpec(memory_space=pltpu.SMEM)
VMEM_BYTES = 66_000_000
META = 128
TOK_STEP = 16
FF_CHUNK = 512
LOOKAHEAD = 3
OWN_FIRST = 5
PASS_CHUNK = 2048
SHARED_CHUNK = 512
SHARED_RING = 2
Q_CHUNK = 512
CHIP_CORES = 2
ROW_TILE = 128


def rms(vals):
    return vals * lax.rsqrt(jnp.mean(vals * vals, axis=-1, keepdims=True) + RMS_EPS)


def mm(lhs, rhs):
    return jnp.dot(lhs, rhs, preferred_element_type=F32)


def silu(vals):
    return vals * (1.0 / (1.0 + jnp.exp(-vals)))


def attention_kernel(layer, capacity, q_heads, kv_heads, lens, x_ref, row_len_ref, ids_ref, wr_ref, wq, wk, wv, wo, kc, vc,
                     a_ref, u_ref, meta_ref, wq_b, wk_b, wv_b, wo_b, k_b, v_b, q3, kn3, vn3, o3, attn, w_sem, q_sem, k_sem, v_sem):
    n_tok, d_model = x_ref.shape
    rows = kc.shape[2]
    head_dim = kc.shape[3]
    group = q_heads // kv_heads
    steps = n_tok // TOK_STEP
    q_steps = q_heads * head_dim // Q_CHUNK
    first = lax.axis_index("pool") * n_tok
    scale = head_dim ** -0.5
    k_copy = pltpu.make_async_copy(wk.at[layer], wk_b, w_sem.at[0])
    v_copy = pltpu.make_async_copy(wv.at[layer], wv_b, w_sem.at[1])
    o_copy = pltpu.make_async_copy(wo.at[layer], wo_b, w_sem.at[2])

    def q_copy(step):
        cols = pl.ds(step * Q_CHUNK, Q_CHUNK)
        return pltpu.make_async_copy(wq.at[layer, :, cols], wq_b.at[:, cols], q_sem.at[step])

    def cache_copies(step):
        here = pl.ds(step * TOK_STEP, TOK_STEP)
        there = pl.ds(first + step * TOK_STEP, TOK_STEP)
        return (pltpu.make_async_copy(kc.at[layer, there], k_b.at[here], k_sem.at[step]),
                pltpu.make_async_copy(vc.at[layer, there], v_b.at[here], v_sem.at[step]))

    def start_cache(step):
        for copy in cache_copies(step):
            copy.start()

    k_copy.start()
    v_copy.start()
    q_copy(0).start()

    q3[:, q_heads:, :] = jnp.zeros((n_tok, q3.shape[1] - q_heads, head_dim), F32)
    kn3[:, q_heads:, :] = jnp.zeros((n_tok, q3.shape[1] - q_heads, head_dim), F32)
    vn3[:, q_heads:, :] = jnp.zeros((n_tok, q3.shape[1] - q_heads, head_dim), F32)
    all_tok = row_len_ref.shape[1]
    mine = lax.broadcasted_iota(jnp.int32, (n_tok, all_tok), 1) == first + lax.broadcasted_iota(jnp.int32, (n_tok, all_tok), 0)

    def column(row):
        return jnp.sum(jnp.where(mine, row.astype(F32), 0.0), axis=-1, keepdims=True)

    x_f = x_ref[...].astype(F32)
    hidden = rms(x_f).astype(BF16)
    lane_d = lax.broadcasted_iota(jnp.int32, (n_tok, head_dim), 1)
    half = head_dim // 2
    inv_freq = jnp.exp(lax.rem(lane_d, half).astype(F32) * (-math.log(ROPE_BASE) / half))
    angle = column(row_len_ref[...]) * inv_freq
    cosine = jnp.cos(angle)
    sine = jnp.sin(angle)
    sine = jnp.where(lane_d < half, -sine, sine)

    def rotated(vals):
        return (vals * cosine + pltpu.roll(vals, half, 1) * sine).astype(BF16).astype(F32)

    k_copy.wait()
    q_copy(1).start()
    key = mm(hidden, wk_b[...])
    v_copy.wait()
    q_copy(2).start()
    val = mm(hidden, wv_b[...]).astype(BF16).astype(F32)
    for kv in range(kv_heads):
        cols = slice(kv * head_dim, (kv + 1) * head_dim)
        key_rot = rotated(key[:, cols])
        for head in range(kv * group, (kv + 1) * group):
            kn3[:, head, :] = key_rot
            vn3[:, head, :] = val[:, cols]
    for step in range(q_steps):
        q_copy(step).wait()
        start_cache(step)
        query = mm(hidden, wq_b[:, step * Q_CHUNK:(step + 1) * Q_CHUNK])
        for i in range(Q_CHUNK // head_dim):
            q3[:, step * (Q_CHUNK // head_dim) + i, :] = rotated(query[:, i * head_dim:(i + 1) * head_dim])
    for step in range(q_steps, steps):
        start_cache(step)
    o_copy.start()

    pad = q3.shape[1]
    lane = lax.broadcasted_iota(jnp.int32, (pad, rows), 1)
    head_kv = lax.broadcasted_iota(jnp.int32, (pad, rows), 0) // group
    right_kv = lane % kv_heads == head_kv
    position = lane // kv_heads

    def step_body(step, carry):
        for copy in cache_copies(step):
            copy.wait()
        base = step * TOK_STEP
        q_f = q3[pl.ds(base, TOK_STEP)]
        scores = lax.dot_general(q_f.astype(BF16), k_b[pl.ds(base, TOK_STEP)], (((2,), (2,)), ((0,), (0,))), preferred_element_type=F32)
        s_new = jnp.sum(q_f * kn3[pl.ds(base, TOK_STEP)], axis=-1, keepdims=True) * scale
        probs = []
        p_news = []
        for i in range(TOK_STEP):
            valid = right_kv & (position < lens[first + base + i])
            s_i = jnp.where(valid, scores[i] * scale, -jnp.inf)
            peak = jnp.maximum(jnp.max(s_i, axis=-1, keepdims=True), s_new[i])
            e_i = jnp.exp(s_i - peak)
            e_new = jnp.exp(s_new[i] - peak)
            total = jnp.sum(e_i, axis=-1, keepdims=True) + e_new
            probs.append((e_i / total).astype(BF16))
            p_news.append((e_new / total).astype(BF16).astype(F32))
        for i in range(TOK_STEP):
            mixed = mm(probs[i], v_b[base + i])
            o3[base + i] = mixed + p_news[i] * vn3[base + i]
        return carry

    lax.fori_loop(0, steps, step_body, 0)
    for head in range(q_heads):
        attn[:, head * head_dim:(head + 1) * head_dim] = o3[:, head, :].astype(BF16)
    o_copy.wait()
    resid = (x_f + mm(attn[...], wo_b[...])).astype(BF16)
    a_ref[...] = resid
    normed = rms(resid.astype(F32)).astype(BF16)
    u_ref[:, :d_model] = normed

    logits = lax.dot_general(normed.astype(F32), wr_ref[layer], (((1,), (1,)), ((), ())), precision=lax.Precision.HIGHEST, preferred_element_type=F32)
    experts = logits.shape[1]
    lane_e = lax.broadcasted_iota(jnp.int32, (n_tok, META), 1).astype(F32)
    id0 = column(ids_ref[layer, 0:1, :])
    id1 = column(ids_ref[layer, 1:2, :])
    pick0 = lane_e == id0
    pick1 = lane_e == id1
    l0 = jnp.sum(jnp.where(pick0[:, :experts], logits, 0.0), axis=-1, keepdims=True)
    l1 = jnp.sum(jnp.where(pick1[:, :experts], logits, 0.0), axis=-1, keepdims=True)
    peak = jnp.maximum(l0, l1)
    e0 = jnp.exp(l0 - peak)
    e1 = jnp.exp(l1 - peak)
    member = jnp.where(pick0 | pick1, 1.0, 0.0)
    earlier = jnp.where(lax.broadcasted_iota(jnp.int32, (n_tok, n_tok), 1) < lax.broadcasted_iota(jnp.int32, (n_tok, n_tok), 0), 1.0, 0.0)
    rank = mm(earlier.astype(BF16), member.astype(BF16))
    u_ref[:, d_model:] = jnp.where(member > 0.0, rank, -1.0).astype(BF16)
    slot0 = id0 * capacity + jnp.sum(jnp.where(pick0, rank, 0.0), axis=-1, keepdims=True)
    slot1 = id1 * capacity + jnp.sum(jnp.where(pick1, rank, 0.0), axis=-1, keepdims=True)
    total = e0 + e1
    meta_ref[...] = jnp.where(lane_e == 0, slot0, jnp.where(lane_e == 1, slot1, jnp.where(lane_e == 2, e0 / total, e1 / total)))


def row_blocks(capacity, blocks=((0, 2), (2, 4), (4, 8))):
    sizes = [-(-(hi - lo) * capacity // ROW_TILE) * ROW_TILE if (hi - lo) * capacity < ROW_TILE else (hi - lo) * capacity for lo, hi in blocks]
    return [sum(sizes[:i]) for i in range(len(sizes))], sizes


def moe_kernel(layer, capacity, ep_size, u_ref, a_ref, meta_ref, sg, su, sd, wg, wu, wd, out_ref,
               gath, back, picked, sent, acc_e, acc_s, pair, other_s, g_w, u_w, d_w, g_b, u_b, d_b, e_sem, s_sem, ag_send, ag_recv, ret_send, ret_recv, sum_send, sum_recv):
    n_tok = a_ref.shape[0]
    d_model = a_ref.shape[1]
    half = n_tok // 2
    e_chunks = wg.shape[3] // FF_CHUNK
    s_chunks = sg.shape[2] // (SHARED_CHUNK * CHIP_CORES)
    me = lax.axis_index("ep")
    partner = me + 1 - 2 * lax.rem(me, 2)
    right = lax.rem(me + 2, ep_size)
    left = lax.rem(me + ep_size - 2, ep_size)
    far = lax.rem(me + ep_size // 2, ep_size)
    p_right = lax.rem(partner + 2, ep_size)
    p_left = lax.rem(partner + ep_size - 2, ep_size)
    p_far = lax.rem(partner + ep_size // 2, ep_size)
    places = [me, partner, far, p_far, right, p_right, left, p_left]
    blocks = [(0, 2), (2, 4), (4, 8)]
    starts, sizes = row_blocks(capacity, blocks)
    row_of = {place: starts[i] + (place - lo) * capacity for i, (lo, hi) in enumerate(blocks) for place in range(lo, hi)}

    def expert_copies(chunk):
        cols = pl.ds(chunk * FF_CHUNK, FF_CHUNK)
        pairs = ((wg.at[layer, 0, :, cols], g_w.at[:, cols]), (wu.at[layer, 0, :, cols], u_w.at[:, cols]), (wd.at[layer, 0, cols], d_w.at[cols]))
        return [pltpu.make_async_copy(src, dst, e_sem.at[chunk, i]) for i, (src, dst) in enumerate(pairs)]

    s_first = lax.rem(me, CHIP_CORES) * s_chunks

    def shared_copies(chunk, slot):
        cols = pl.ds((s_first + chunk) * SHARED_CHUNK, SHARED_CHUNK)
        pairs = ((sg.at[layer, :, cols], g_b.at[slot]), (su.at[layer, :, cols], u_b.at[slot]), (sd.at[layer, cols], d_b.at[slot]))
        return [pltpu.make_async_copy(src, dst, s_sem.at[slot, i]) for i, (src, dst) in enumerate(pairs)]

    for chunk in range(LOOKAHEAD):
        for copy in expert_copies(chunk):
            copy.start()

    barrier = pltpu.get_barrier_semaphore()
    for other in range(1, ep_size):
        pl.semaphore_signal(barrier, inc=1, device_id={"ep": lax.rem(me + other, ep_size)}, device_id_type=MESH)
    gath[me] = u_ref[...]
    pl.semaphore_wait(barrier, ep_size - 1)

    def piece(src, part):
        return gath.at[src, pl.ds(part * half, half)]

    def arrived(src, part):
        pltpu.make_async_remote_copy(src_ref=piece(src, part), dst_ref=piece(src, part), send_sem=ag_send.at[0], recv_sem=ag_recv.at[src, part],
                                     device_id={"ep": partner}, device_id_type=MESH).wait_recv()

    sends = []

    def send(src, part, target, from_input=False):
        ref = u_ref.at[pl.ds(part * half, half)] if from_input else piece(src, part)
        copy = pltpu.make_async_remote_copy(src_ref=ref, dst_ref=piece(src, part), send_sem=ag_send.at[len(sends)], recv_sem=ag_recv.at[src, part],
                                            device_id={"ep": target}, device_id_type=MESH)
        copy.start()
        sends.append(copy)

    send(me, 0, partner, True)
    send(me, 1, partner, True)
    send(me, 0, right, True)
    send(me, 1, left, True)
    send(me, 1, right, True)
    send(me, 0, left, True)

    acc_s[...] = jnp.zeros_like(acc_s)
    acc_e[...] = jnp.zeros_like(acc_e)
    picked[...] = jnp.zeros_like(picked)
    lane = lax.broadcasted_iota(jnp.int32, (n_tok, META), 1)

    def pick(src, codes, values, place):
        rank = jnp.sum(jnp.where(lane == me, codes.astype(F32), 0.0), axis=-1, keepdims=True)
        choose = jnp.where(lane.astype(F32) == rank, 1.0, 0.0).astype(BF16)
        rows = lax.dot_general(choose, values, (((0,), (0,)), ((), ())), preferred_element_type=F32)
        picked[pl.ds(row_of[place], capacity)] = rows[:capacity].astype(BF16)

    def pick_places(first, last):
        for place in range(first, last):
            src = places[place]
            if place == 0:
                pick(src, u_ref[:, d_model:], u_ref[:, :d_model], place)
            else:
                pick(src, gath[src, :, d_model:], gath[src, :, :d_model], place)

    def expert_rows(block, chunk, width):
        rows = pl.ds(starts[block], sizes[block])
        cols = pl.ds(pl.multiple_of(chunk * width, width), width)
        x_rows = picked[rows]
        mid = (silu(mm(x_rows, g_w[:, cols])) * mm(x_rows, u_w[:, cols])).astype(BF16)
        acc_e[rows] += mm(mid, d_w[cols])

    def return_copy(place):
        target = places[place]
        return pltpu.make_async_remote_copy(src_ref=sent.at[place], dst_ref=back.at[me], send_sem=ret_send.at[place], recv_sem=ret_recv.at[me],
                                            device_id={"ep": target}, device_id_type=MESH)

    def give_back(first, last):
        for place in range(first, last):
            sent[place] = acc_e[pl.ds(row_of[place], capacity)].astype(BF16)
        for place in range(max(first, 1), last):
            return_copy(place).start()

    def own_step(chunk, carry):
        for copy in expert_copies(chunk):
            copy.wait()

        @pl.when(chunk + LOOKAHEAD < e_chunks)
        def _():
            for copy in expert_copies(chunk + LOOKAHEAD):
                copy.start()

        expert_rows(0, chunk, FF_CHUNK)
        return carry

    for part in (0, 1):
        arrived(partner, part)
    pick_places(0, 2)
    lax.fori_loop(0, 2, own_step, 0)
    arrived(left, 0)
    send(left, 0, right)
    arrived(right, 1)
    send(right, 1, left)
    send(left, 0, partner)
    send(right, 1, partner)
    lax.fori_loop(2, 4, own_step, 0)
    for src, part in ((left, 1), (right, 0)):
        arrived(src, part)
        send(src, part, partner)
    lax.fori_loop(4, OWN_FIRST, own_step, 0)
    for slot in range(SHARED_RING):
        for copy in shared_copies(slot, slot):
            copy.start()
    for src in (p_right, p_left):
        for part in (0, 1):
            arrived(src, part)
    pick_places(4, 8)
    per_step = PASS_CHUNK // FF_CHUNK
    sent_before = len(sends)

    def far_copy(part):
        return pltpu.make_async_remote_copy(src_ref=piece(far, part), dst_ref=piece(far, part), send_sem=ag_send.at[sent_before + part],
                                            recv_sem=ag_recv.at[far, part], device_id={"ep": partner}, device_id_type=MESH)


    def near_step(step, carry):
        for chunk in range(OWN_FIRST, e_chunks):

            @pl.when(step == chunk // per_step)
            def _():
                for copy in expert_copies(chunk):
                    copy.wait()

        expert_rows(2, step, PASS_CHUNK)

        @pl.when(step == 0)
        def _():
            for part in (0, 1):
                arrived(far, part)
                far_copy(part).start()

        return carry

    lax.fori_loop(0, e_chunks // per_step, near_step, 0)
    give_back(4, 8)
    for src in (p_far,):
        for part in (0, 1):
            arrived(src, part)
    pick_places(2, 4)

    def far_step(step, carry):
        expert_rows(1, step, PASS_CHUNK)
        return carry

    lax.fori_loop(0, e_chunks // per_step, far_step, 0)
    give_back(2, 4)

    def own_rest(chunk, carry):
        expert_rows(0, chunk, FF_CHUNK)
        return carry

    lax.fori_loop(OWN_FIRST, e_chunks, own_rest, 0)
    give_back(0, 2)
    pair[pl.ds(0, n_tok)] = u_ref[:, :d_model]
    pair[pl.ds(n_tok, n_tok)] = gath[partner, :, :d_model]

    def shared_step(chunk, carry):
        slot = lax.rem(chunk, SHARED_RING)
        for copy in shared_copies(chunk, slot):
            copy.wait()
        rows = pair[...]
        mid = (silu(mm(rows, g_b[slot])) * mm(rows, u_b[slot])).astype(BF16)
        acc_s[...] += mm(mid, d_b[slot])

        @pl.when(chunk + SHARED_RING < s_chunks)
        def _():
            for copy in shared_copies(chunk + SHARED_RING, slot):
                copy.start()

        return carry

    lax.fori_loop(0, s_chunks, shared_step, 0)
    sum_copy = pltpu.make_async_remote_copy(src_ref=acc_s.at[pl.ds(n_tok, n_tok)], dst_ref=other_s, send_sem=sum_send, recv_sem=sum_recv,
                                            device_id={"ep": partner}, device_id_type=MESH)
    sum_copy.start()
    back[me] = sent[0]
    for copy in sends + [far_copy(0), far_copy(1)]:
        copy.wait_send()
    for place in range(1, ep_size):
        return_copy(place).wait_send()
        src = places[place]
        pltpu.make_async_remote_copy(src_ref=back.at[src], dst_ref=back.at[src], send_sem=ret_send.at[place], recv_sem=ret_recv.at[src],
                                     device_id={"ep": src}, device_id_type=MESH).wait_recv()

    slot_lane = lax.broadcasted_iota(jnp.int32, (n_tok, ep_size * capacity), 1).astype(F32)
    table = back[...].reshape(ep_size * capacity, d_model)
    choose = jnp.concatenate([jnp.where(slot_lane == meta_ref[:, 0:1], 1.0, 0.0), jnp.where(slot_lane == meta_ref[:, 1:2], 1.0, 0.0)], axis=0).astype(BF16)
    y_pair = mm(choose, table)
    routed = meta_ref[:, 2:3] * y_pair[:n_tok] + meta_ref[:, 3:4] * y_pair[n_tok:]
    sum_copy.wait()
    shared_out = (acc_s[pl.ds(0, n_tok)] + other_s[...]).astype(BF16).astype(F32)
    out_ref[...] = (a_ref[...].astype(F32) + routed + shared_out).astype(BF16)


def solution(mesh):
    ep_size = mesh.shape["ep"]
    row_spec = P(("dp", "ep", "pool"), None)
    cache_spec = P(None, ("dp", "ep"), None, None, None)
    expert_spec = P(None, "ep", None, None)
    in_specs = (row_spec, cache_spec, cache_spec, P(("dp", "ep")), P(), P(), P(), P(), P(), P(None, ("dp", "ep"), None), expert_spec, expert_spec, expert_spec, P(), P(), P())

    def body(x_loc, k_cache, v_cache, cache_len, w_query, w_key, w_value, w_out, w_router, expert_ids, w_gate, w_up, w_down, shared_gate, shared_up, shared_down):
        n_tok, d_model = x_loc.shape
        n_layers, all_tok, ctx, kv_heads, head_dim = k_cache.shape
        q_heads = w_query.shape[2] // head_dim
        top_k = expert_ids.shape[2]
        capacity = 3 * n_tok * top_k // ep_size
        rows = ctx * kv_heads
        pad_heads = -(-q_heads // 8) * 8
        ids_t = jnp.swapaxes(expert_ids, 1, 2)
        row_len = cache_len.reshape(1, cache_len.shape[0])
        router_t = jnp.swapaxes(w_router, 1, 2)
        k_rows = k_cache.reshape(n_layers, all_tok, rows, head_dim)
        v_rows = v_cache.reshape(n_layers, all_tok, rows, head_dim)
        ext = d_model + META
        n_rows = sum(row_blocks(capacity)[1])
        x_cur = x_loc
        for layer in range(n_layers):
            resid, u_ext, meta = pl.pallas_call(
                functools.partial(attention_kernel, layer, capacity, q_heads, kv_heads),
                name=f"attention_{layer}",
                out_shape=(jax.ShapeDtypeStruct((n_tok, d_model), BF16), jax.ShapeDtypeStruct((n_tok, ext), BF16), jax.ShapeDtypeStruct((n_tok, META), F32)),
                in_specs=[SMEM] + [VMEM] * 4 + [ANY] * 6,
                out_specs=(VMEM, VMEM, VMEM),
                scratch_shapes=[
                    pltpu.VMEM(w_query.shape[1:], BF16), pltpu.VMEM(w_key.shape[1:], BF16), pltpu.VMEM(w_value.shape[1:], BF16), pltpu.VMEM(w_out.shape[1:], BF16),
                    pltpu.VMEM((n_tok, rows, head_dim), BF16), pltpu.VMEM((n_tok, rows, head_dim), BF16),
                    pltpu.VMEM((n_tok, pad_heads, head_dim), F32), pltpu.VMEM((n_tok, pad_heads, head_dim), F32),
                    pltpu.VMEM((n_tok, pad_heads, head_dim), F32), pltpu.VMEM((n_tok, pad_heads, head_dim), F32),
                    pltpu.VMEM((n_tok, q_heads * head_dim), BF16),
                    pltpu.SemaphoreType.DMA((3,)), pltpu.SemaphoreType.DMA((q_heads * head_dim // Q_CHUNK,)), pltpu.SemaphoreType.DMA((n_tok // TOK_STEP,)), pltpu.SemaphoreType.DMA((n_tok // TOK_STEP,)),
                ],
                compiler_params=pltpu.CompilerParams(vmem_limit_bytes=VMEM_BYTES),
            )(cache_len, x_cur, row_len, ids_t, router_t, w_query, w_key, w_value, w_out, k_rows, v_rows)
            x_cur = pl.pallas_call(
                functools.partial(moe_kernel, layer, capacity, ep_size),
                name=f"moe_{layer}",
                out_shape=jax.ShapeDtypeStruct((n_tok, d_model), BF16),
                in_specs=[VMEM] * 3 + [ANY] * 6,
                out_specs=VMEM,
                scratch_shapes=[
                    pltpu.VMEM((ep_size, n_tok, ext), BF16), pltpu.VMEM((ep_size, capacity, d_model), BF16),
                    pltpu.VMEM((n_rows, d_model), BF16), pltpu.VMEM((ep_size, capacity, d_model), BF16),
                    pltpu.VMEM((n_rows, d_model), F32), pltpu.VMEM((CHIP_CORES * n_tok, d_model), F32),
                    pltpu.VMEM((CHIP_CORES * n_tok, d_model), BF16), pltpu.VMEM((n_tok, d_model), F32),
                    pltpu.VMEM(w_gate.shape[2:], BF16), pltpu.VMEM(w_up.shape[2:], BF16), pltpu.VMEM(w_down.shape[2:], BF16),
                    pltpu.VMEM((SHARED_RING, d_model, SHARED_CHUNK), BF16), pltpu.VMEM((SHARED_RING, d_model, SHARED_CHUNK), BF16), pltpu.VMEM((SHARED_RING, SHARED_CHUNK, d_model), BF16),
                    pltpu.SemaphoreType.DMA((w_gate.shape[3] // FF_CHUNK, 3)), pltpu.SemaphoreType.DMA((SHARED_RING, 3)), pltpu.SemaphoreType.DMA((14,)), pltpu.SemaphoreType.DMA((ep_size, 2)),
                    pltpu.SemaphoreType.DMA((ep_size,)), pltpu.SemaphoreType.DMA((ep_size,)), pltpu.SemaphoreType.DMA, pltpu.SemaphoreType.DMA,
                ],
                compiler_params=pltpu.CompilerParams(vmem_limit_bytes=VMEM_BYTES, collective_id=layer, has_side_effects=True),
            )(u_ext, resid, meta, shared_gate, shared_up, shared_down, w_gate, w_up, w_down)
        return x_cur

    return jax.shard_map(body, mesh=mesh, in_specs=in_specs, out_specs=row_spec, check_vma=False)
```

```python
import functools
import math
import jax
import jax.numpy as jnp
from jax import lax
from jax.experimental import pallas as pl
from jax.experimental.pallas import tpu as pltpu
from jax.sharding import PartitionSpec as P

RMS_EPS = 1e-6
ROPE_BASE = 10000.0
MESH = pl.DeviceIdType.MESH
BF16 = jnp.bfloat16
F32 = jnp.float32
ANY = pl.BlockSpec(memory_space=pl.ANY)
VMEM = pl.BlockSpec(memory_space=pltpu.VMEM)
SMEM = pl.BlockSpec(memory_space=pltpu.SMEM)
VMEM_BYTES = 66_000_000
META = 128
TOK_STEP = 16
FF_CHUNK = 512
LOOKAHEAD = 3
OWN_FIRST = 4
PASS_CHUNK = 2048
SHARED_CHUNK = 512
SHARED_RING = 2
Q_CHUNK = 512
CHIP_CORES = 2


def rms(vals):
    return vals * lax.rsqrt(jnp.mean(vals * vals, axis=-1, keepdims=True) + RMS_EPS)


def mm(lhs, rhs):
    return jnp.dot(lhs, rhs, preferred_element_type=F32)


def silu(vals):
    return vals * (1.0 / (1.0 + jnp.exp(-vals)))


def attention_kernel(layer, capacity, q_heads, kv_heads, lens, x_ref, row_len_ref, ids_ref, wr_ref, wq, wk, wv, wo, kc, vc,
                     a_ref, u_ref, meta_ref, x_v, wr_v, wr_parts, wq_b, wk_b, wv_b, wo_b, k_b, v_b, q3, kn3, vn3, o3, attn, in_sem, w_sem, q_sem, k_sem, v_sem):
    n_tok, d_model = x_ref.shape
    rows = kc.shape[2]
    head_dim = kc.shape[3]
    group = q_heads // kv_heads
    steps = n_tok // TOK_STEP
    q_steps = q_heads * head_dim // Q_CHUNK
    first = lax.axis_index("pool") * n_tok
    scale = head_dim ** -0.5
    k_copy = pltpu.make_async_copy(wk.at[layer], wk_b, w_sem.at[0])
    v_copy = pltpu.make_async_copy(wv.at[layer], wv_b, w_sem.at[1])
    o_copy = pltpu.make_async_copy(wo.at[layer], wo_b, w_sem.at[2])

    def q_copy(step):
        cols = pl.ds(step * Q_CHUNK, Q_CHUNK)
        return pltpu.make_async_copy(wq.at[layer, :, cols], wq_b.at[:, cols], q_sem.at[step])

    def cache_copies(step):
        here = pl.ds(step * TOK_STEP, TOK_STEP)
        there = pl.ds(first + step * TOK_STEP, TOK_STEP)
        return (pltpu.make_async_copy(kc.at[layer, there], k_b.at[here], k_sem.at[step]),
                pltpu.make_async_copy(vc.at[layer, there], v_b.at[here], v_sem.at[step]))

    def start_cache(step):
        for copy in cache_copies(step):
            copy.start()

    x_copy = pltpu.make_async_copy(x_ref, x_v, in_sem.at[0])
    wr_copy = pltpu.make_async_copy(wr_ref.at[layer], wr_v, in_sem.at[1])
    x_copy.start()
    wr_copy.start()
    k_copy.start()
    v_copy.start()
    q_copy(0).start()

    q3[:, q_heads:, :] = jnp.zeros((n_tok, q3.shape[1] - q_heads, head_dim), F32)
    kn3[:, q_heads:, :] = jnp.zeros((n_tok, q3.shape[1] - q_heads, head_dim), F32)
    vn3[:, q_heads:, :] = jnp.zeros((n_tok, q3.shape[1] - q_heads, head_dim), F32)
    experts = wr_v.shape[0]
    all_tok = row_len_ref.shape[1]
    mine = lax.broadcasted_iota(jnp.int32, (n_tok, all_tok), 1) == first + lax.broadcasted_iota(jnp.int32, (n_tok, all_tok), 0)

    def column(row):
        return jnp.sum(jnp.where(mine, row.astype(F32), 0.0), axis=-1, keepdims=True)

    x_copy.wait()
    x_f = x_v[...].astype(F32)
    hidden = rms(x_f).astype(BF16)
    lane_d = lax.broadcasted_iota(jnp.int32, (n_tok, head_dim), 1)
    half = head_dim // 2
    inv_freq = jnp.exp(lax.rem(lane_d, half).astype(F32) * (-math.log(ROPE_BASE) / half))
    angle = column(row_len_ref[...]) * inv_freq
    cosine = jnp.cos(angle)
    sine = jnp.sin(angle)
    sine = jnp.where(lane_d < half, -sine, sine)

    def rotated(vals):
        return (vals * cosine + pltpu.roll(vals, half, 1) * sine).astype(BF16).astype(F32)

    wr_copy.wait()
    coarse = wr_v[...].astype(BF16)
    rest = wr_v[...] - coarse.astype(F32)
    middle = rest.astype(BF16)
    fine = (rest - middle.astype(F32)).astype(BF16)
    wr_parts[0:experts] = coarse.astype(F32)
    wr_parts[experts:2 * experts] = middle.astype(F32)
    wr_parts[2 * experts:3 * experts] = fine.astype(F32)
    k_copy.wait()
    q_copy(1).start()
    key = mm(hidden, wk_b[...])
    v_copy.wait()
    q_copy(2).start()
    val = mm(hidden, wv_b[...]).astype(BF16).astype(F32)
    for kv in range(kv_heads):
        cols = slice(kv * head_dim, (kv + 1) * head_dim)
        key_rot = rotated(key[:, cols])
        for head in range(kv * group, (kv + 1) * group):
            kn3[:, head, :] = key_rot
            vn3[:, head, :] = val[:, cols]
    for step in range(q_steps):
        q_copy(step).wait()
        start_cache(step)
        query = mm(hidden, wq_b[:, step * Q_CHUNK:(step + 1) * Q_CHUNK])
        for i in range(Q_CHUNK // head_dim):
            q3[:, step * (Q_CHUNK // head_dim) + i, :] = rotated(query[:, i * head_dim:(i + 1) * head_dim])
    for step in range(q_steps, steps):
        start_cache(step)
    o_copy.start()

    pad = q3.shape[1]
    lane = lax.broadcasted_iota(jnp.int32, (pad, rows), 1)
    head_kv = lax.broadcasted_iota(jnp.int32, (pad, rows), 0) // group
    right_kv = lane % kv_heads == head_kv
    position = lane // kv_heads

    def step_body(step, carry):
        for copy in cache_copies(step):
            copy.wait()
        base = step * TOK_STEP
        q_f = q3[pl.ds(base, TOK_STEP)]
        scores = lax.dot_general(q_f.astype(BF16), k_b[pl.ds(base, TOK_STEP)], (((2,), (2,)), ((0,), (0,))), preferred_element_type=F32)
        s_new = jnp.sum(q_f * kn3[pl.ds(base, TOK_STEP)], axis=-1, keepdims=True) * scale
        probs = []
        p_news = []
        for i in range(TOK_STEP):
            valid = right_kv & (position < lens[first + base + i])
            s_i = jnp.where(valid, scores[i] * scale, -jnp.inf)
            peak = jnp.maximum(jnp.max(s_i, axis=-1, keepdims=True), s_new[i])
            e_i = jnp.exp(s_i - peak)
            e_new = jnp.exp(s_new[i] - peak)
            total = jnp.sum(e_i, axis=-1, keepdims=True) + e_new
            probs.append((e_i / total).astype(BF16))
            p_news.append((e_new / total).astype(BF16).astype(F32))
        for i in range(TOK_STEP):
            mixed = mm(probs[i], v_b[base + i])
            o3[base + i] = mixed + p_news[i] * vn3[base + i]
        return carry

    lax.fori_loop(0, steps, step_body, 0)
    for head in range(q_heads):
        attn[:, head * head_dim:(head + 1) * head_dim] = o3[:, head, :].astype(BF16)
    o_copy.wait()
    resid = (x_f + mm(attn[...], wo_b[...])).astype(BF16)
    a_ref[...] = resid
    normed = rms(resid.astype(F32)).astype(BF16)
    u_ref[:, :d_model] = normed

    logits = lax.dot_general(normed, wr_parts[...].astype(BF16), (((1,), (1,)), ((), ())), preferred_element_type=F32)
    column_id = lax.broadcasted_iota(jnp.int32, logits.shape, 1)
    column_id = lax.rem(column_id, experts).astype(F32)
    lane_e = lax.broadcasted_iota(jnp.int32, (n_tok, META), 1).astype(F32)
    id0 = column(ids_ref[layer, 0:1, :])
    id1 = column(ids_ref[layer, 1:2, :])
    pick0 = lane_e == id0
    pick1 = lane_e == id1
    l0 = jnp.sum(jnp.where(column_id == id0, logits, 0.0), axis=-1, keepdims=True)
    l1 = jnp.sum(jnp.where(column_id == id1, logits, 0.0), axis=-1, keepdims=True)
    peak = jnp.maximum(l0, l1)
    e0 = jnp.exp(l0 - peak)
    e1 = jnp.exp(l1 - peak)
    member = jnp.where(pick0 | pick1, 1.0, 0.0)
    earlier = jnp.where(lax.broadcasted_iota(jnp.int32, (n_tok, n_tok), 1) < lax.broadcasted_iota(jnp.int32, (n_tok, n_tok), 0), 1.0, 0.0)
    rank = mm(earlier.astype(BF16), member.astype(BF16))
    u_ref[:, d_model:] = jnp.where(member > 0.0, rank, -1.0).astype(BF16)
    slot0 = id0 * capacity + jnp.sum(jnp.where(pick0, rank, 0.0), axis=-1, keepdims=True)
    slot1 = id1 * capacity + jnp.sum(jnp.where(pick1, rank, 0.0), axis=-1, keepdims=True)
    total = e0 + e1
    meta_ref[...] = jnp.where(lane_e == 0, slot0, jnp.where(lane_e == 1, slot1, jnp.where(lane_e == 2, e0 / total, e1 / total)))


def moe_kernel(layer, capacity, ep_size, u_hbm, a_hbm, meta_hbm, sg, su, sd, wg, wu, wd, out_ref,
               u_ref, a_ref, meta_ref, gath, back, picked, sent, acc_e, acc_s, pair, other_s, g_w, u_w, d_w, g_b, u_b, d_b, e_sem, s_sem, ag_send, ag_recv, ret_send, ret_recv, sum_send, sum_recv, in_sem):
    n_tok = a_ref.shape[0]
    d_model = a_ref.shape[1]
    half = n_tok // 2
    e_chunks = wg.shape[3] // FF_CHUNK
    s_chunks = sg.shape[2] // (SHARED_CHUNK * CHIP_CORES)
    me = lax.axis_index("ep")
    partner = me + 1 - 2 * lax.rem(me, 2)
    right = lax.rem(me + 2, ep_size)
    left = lax.rem(me + ep_size - 2, ep_size)
    far = lax.rem(me + ep_size // 2, ep_size)
    p_right = lax.rem(partner + 2, ep_size)
    p_left = lax.rem(partner + ep_size - 2, ep_size)
    p_far = lax.rem(partner + ep_size // 2, ep_size)
    places = [me, partner, far, p_far, right, p_right, left, p_left]

    def expert_copies(chunk):
        cols = pl.ds(chunk * FF_CHUNK, FF_CHUNK)
        pairs = ((wg.at[layer, 0, :, cols], g_w.at[:, cols]), (wu.at[layer, 0, :, cols], u_w.at[:, cols]), (wd.at[layer, 0, cols], d_w.at[cols]))
        return [pltpu.make_async_copy(src, dst, e_sem.at[chunk, i]) for i, (src, dst) in enumerate(pairs)]

    s_first = lax.rem(me, CHIP_CORES) * s_chunks

    def shared_copies(chunk, slot):
        cols = pl.ds((s_first + chunk) * SHARED_CHUNK, SHARED_CHUNK)
        pairs = ((sg.at[layer, :, cols], g_b.at[slot]), (su.at[layer, :, cols], u_b.at[slot]), (sd.at[layer, cols], d_b.at[slot]))
        return [pltpu.make_async_copy(src, dst, s_sem.at[slot, i]) for i, (src, dst) in enumerate(pairs)]

    in_copies = [pltpu.make_async_copy(src, dst, in_sem.at[i]) for i, (src, dst) in enumerate(((u_hbm, u_ref), (a_hbm, a_ref), (meta_hbm, meta_ref)))]
    in_copies[0].start()
    for chunk in range(LOOKAHEAD):
        for copy in expert_copies(chunk):
            copy.start()
    for copy in in_copies[1:]:
        copy.start()

    barrier = pltpu.get_barrier_semaphore()
    for other in range(1, ep_size):
        pl.semaphore_signal(barrier, inc=1, device_id={"ep": lax.rem(me + other, ep_size)}, device_id_type=MESH)
    in_copies[0].wait()
    pl.semaphore_wait(barrier, ep_size - 1)

    def piece(src, part):
        return gath.at[src, pl.ds(part * half, half)]

    def arrived(src, part):
        pltpu.make_async_remote_copy(src_ref=piece(src, part), dst_ref=piece(src, part), send_sem=ag_send.at[0], recv_sem=ag_recv.at[src, part],
                                     device_id={"ep": partner}, device_id_type=MESH).wait_recv()

    sends = []

    def send(src, part, target, from_input=False):
        ref = u_ref.at[pl.ds(part * half, half)] if from_input else piece(src, part)
        copy = pltpu.make_async_remote_copy(src_ref=ref, dst_ref=piece(src, part), send_sem=ag_send.at[len(sends)], recv_sem=ag_recv.at[src, part],
                                            device_id={"ep": target}, device_id_type=MESH)
        copy.start()
        sends.append(copy)

    send(me, 0, partner, True)
    send(me, 1, partner, True)
    send(me, 0, right, True)
    send(me, 1, left, True)
    send(me, 1, right, True)
    send(me, 0, left, True)

    acc_s[...] = jnp.zeros_like(acc_s)
    acc_e[...] = jnp.zeros_like(acc_e)
    lane = lax.broadcasted_iota(jnp.int32, (n_tok, META), 1)

    def pick(src, codes, values, place):
        rank = jnp.sum(jnp.where(lane == me, codes.astype(F32), 0.0), axis=-1, keepdims=True)
        choose = jnp.where(lane.astype(F32) == rank, 1.0, 0.0).astype(BF16)
        rows = lax.dot_general(choose, values, (((0,), (0,)), ((), ())), preferred_element_type=F32)
        picked[pl.ds(place * capacity, capacity)] = rows[:capacity].astype(BF16)

    def pick_places(first, last):
        for place in range(first, last):
            src = places[place]
            if place == 0:
                pick(src, u_ref[:, d_model:], u_ref[:, :d_model], place)
            else:
                pick(src, gath[src, :, d_model:], gath[src, :, :d_model], place)

    def expert_rows(lo, hi, chunk, width):
        rows = pl.ds(lo * capacity, (hi - lo) * capacity)
        cols = pl.ds(pl.multiple_of(chunk * width, width), width)
        x_rows = picked[rows]
        mid = (silu(mm(x_rows, g_w[:, cols])) * mm(x_rows, u_w[:, cols])).astype(BF16)
        acc_e[rows] += mm(mid, d_w[cols])

    def return_copy(place):
        target = places[place]
        return pltpu.make_async_remote_copy(src_ref=sent.at[place], dst_ref=back.at[me], send_sem=ret_send.at[place], recv_sem=ret_recv.at[me],
                                            device_id={"ep": target}, device_id_type=MESH)

    def give_back(first, last):
        for place in range(first, last):
            sent[place] = acc_e[pl.ds(place * capacity, capacity)].astype(BF16)
        for place in range(max(first, 1), last):
            return_copy(place).start()

    def own_step(chunk, carry):
        for copy in expert_copies(chunk):
            copy.wait()

        @pl.when(chunk + LOOKAHEAD < e_chunks)
        def _():
            for copy in expert_copies(chunk + LOOKAHEAD):
                copy.start()

        expert_rows(0, 2, chunk, FF_CHUNK)
        return carry

    for part in (0, 1):
        arrived(partner, part)
    pick_places(0, 2)
    lax.fori_loop(0, 2, own_step, 0)
    arrived(left, 0)
    send(left, 0, right)
    arrived(right, 1)
    send(right, 1, left)
    send(left, 0, partner)
    send(right, 1, partner)
    lax.fori_loop(2, 4, own_step, 0)
    for src, part in ((left, 1), (right, 0)):
        arrived(src, part)
        send(src, part, partner)
    for copy in expert_copies(OWN_FIRST - 1 + LOOKAHEAD + 1) if OWN_FIRST + LOOKAHEAD < e_chunks else ():
        copy.start()
    for slot in range(SHARED_RING):
        for copy in shared_copies(slot, slot):
            copy.start()
    for src in (p_right, p_left):
        for part in (0, 1):
            arrived(src, part)
    pick_places(4, 8)
    per_step = PASS_CHUNK // FF_CHUNK
    sent_before = len(sends)

    def far_copy(part):
        return pltpu.make_async_remote_copy(src_ref=piece(far, part), dst_ref=piece(far, part), send_sem=ag_send.at[sent_before + part],
                                            recv_sem=ag_recv.at[far, part], device_id={"ep": partner}, device_id_type=MESH)


    def near_step(step, carry):
        for chunk in range(OWN_FIRST, e_chunks):

            @pl.when(step == chunk // per_step)
            def _():
                for copy in expert_copies(chunk):
                    copy.wait()

        expert_rows(4, 8, step, PASS_CHUNK)

        @pl.when(step == 0)
        def _():
            for part in (0, 1):
                arrived(far, part)
                far_copy(part).start()

        return carry

    lax.fori_loop(0, e_chunks // per_step, near_step, 0)
    give_back(4, 8)
    for src in (p_far,):
        for part in (0, 1):
            arrived(src, part)
    pick_places(2, 4)

    def far_step(step, carry):
        expert_rows(2, 4, step, PASS_CHUNK)
        return carry

    lax.fori_loop(0, e_chunks // per_step, far_step, 0)
    give_back(2, 4)

    def own_rest(step, carry):
        expert_rows(0, 2, step, PASS_CHUNK)
        return carry

    lax.fori_loop(OWN_FIRST // per_step, e_chunks // per_step, own_rest, 0)
    give_back(0, 2)
    pair[pl.ds(0, n_tok)] = u_ref[:, :d_model]
    pair[pl.ds(n_tok, n_tok)] = gath[partner, :, :d_model]

    def shared_step(chunk, carry):
        slot = lax.rem(chunk, SHARED_RING)
        for copy in shared_copies(chunk, slot):
            copy.wait()
        rows = pair[...]
        mid = (silu(mm(rows, g_b[slot])) * mm(rows, u_b[slot])).astype(BF16)
        acc_s[...] += mm(mid, d_b[slot])

        @pl.when(chunk + SHARED_RING < s_chunks)
        def _():
            for copy in shared_copies(chunk + SHARED_RING, slot):
                copy.start()

        return carry

    lax.fori_loop(0, s_chunks, shared_step, 0)
    sum_copy = pltpu.make_async_remote_copy(src_ref=acc_s.at[pl.ds(n_tok, n_tok)], dst_ref=other_s, send_sem=sum_send, recv_sem=sum_recv,
                                            device_id={"ep": partner}, device_id_type=MESH)
    sum_copy.start()
    back[me] = sent[0]
    for copy in sends + [far_copy(0), far_copy(1)]:
        copy.wait_send()
    for place in range(1, ep_size):
        return_copy(place).wait_send()
        src = places[place]
        pltpu.make_async_remote_copy(src_ref=back.at[src], dst_ref=back.at[src], send_sem=ret_send.at[place], recv_sem=ret_recv.at[src],
                                     device_id={"ep": src}, device_id_type=MESH).wait_recv()

    for copy in in_copies[1:]:
        copy.wait()
    slot_lane = lax.broadcasted_iota(jnp.int32, (n_tok, ep_size * capacity), 1).astype(F32)
    table = back[...].reshape(ep_size * capacity, d_model)
    choose = jnp.concatenate([jnp.where(slot_lane == meta_ref[:, 0:1], 1.0, 0.0), jnp.where(slot_lane == meta_ref[:, 1:2], 1.0, 0.0)], axis=0).astype(BF16)
    y_pair = mm(choose, table)
    routed = meta_ref[:, 2:3] * y_pair[:n_tok] + meta_ref[:, 3:4] * y_pair[n_tok:]
    sum_copy.wait()
    shared_out = (acc_s[pl.ds(0, n_tok)] + other_s[...]).astype(BF16).astype(F32)
    out_ref[...] = (a_ref[...].astype(F32) + routed + shared_out).astype(BF16)


def solution(mesh):
    ep_size = mesh.shape["ep"]
    row_spec = P(("dp", "ep", "pool"), None)
    cache_spec = P(None, ("dp", "ep"), None, None, None)
    expert_spec = P(None, "ep", None, None)
    in_specs = (row_spec, cache_spec, cache_spec, P(("dp", "ep")), P(), P(), P(), P(), P(), P(None, ("dp", "ep"), None), expert_spec, expert_spec, expert_spec, P(), P(), P())

    def body(x_loc, k_cache, v_cache, cache_len, w_query, w_key, w_value, w_out, w_router, expert_ids, w_gate, w_up, w_down, shared_gate, shared_up, shared_down):
        n_tok, d_model = x_loc.shape
        n_layers, all_tok, ctx, kv_heads, head_dim = k_cache.shape
        q_heads = w_query.shape[2] // head_dim
        top_k = expert_ids.shape[2]
        capacity = 3 * n_tok * top_k // ep_size
        rows = ctx * kv_heads
        pad_heads = -(-q_heads // 8) * 8
        ids_t = jnp.swapaxes(expert_ids, 1, 2)
        row_len = cache_len.reshape(1, cache_len.shape[0])
        router_t = jnp.swapaxes(w_router, 1, 2)
        k_rows = k_cache.reshape(n_layers, all_tok, rows, head_dim)
        v_rows = v_cache.reshape(n_layers, all_tok, rows, head_dim)
        ext = d_model + META
        n_rows = ep_size * capacity
        x_cur = x_loc
        for layer in range(n_layers):
            resid, u_ext, meta = pl.pallas_call(
                functools.partial(attention_kernel, layer, capacity, q_heads, kv_heads),
                name=f"attention_{layer}",
                out_shape=(jax.ShapeDtypeStruct((n_tok, d_model), BF16), jax.ShapeDtypeStruct((n_tok, ext), BF16), jax.ShapeDtypeStruct((n_tok, META), F32)),
                in_specs=[SMEM, ANY, VMEM, VMEM] + [ANY] * 7,
                out_specs=(VMEM, VMEM, VMEM),
                scratch_shapes=[
                    pltpu.VMEM((n_tok, d_model), BF16), pltpu.VMEM(router_t.shape[1:], F32), pltpu.VMEM((3 * router_t.shape[1], d_model), F32),
                    pltpu.VMEM(w_query.shape[1:], BF16), pltpu.VMEM(w_key.shape[1:], BF16), pltpu.VMEM(w_value.shape[1:], BF16), pltpu.VMEM(w_out.shape[1:], BF16),
                    pltpu.VMEM((n_tok, rows, head_dim), BF16), pltpu.VMEM((n_tok, rows, head_dim), BF16),
                    pltpu.VMEM((n_tok, pad_heads, head_dim), F32), pltpu.VMEM((n_tok, pad_heads, head_dim), F32),
                    pltpu.VMEM((n_tok, pad_heads, head_dim), F32), pltpu.VMEM((n_tok, pad_heads, head_dim), F32),
                    pltpu.VMEM((n_tok, q_heads * head_dim), BF16),
                    pltpu.SemaphoreType.DMA((2,)), pltpu.SemaphoreType.DMA((3,)), pltpu.SemaphoreType.DMA((q_heads * head_dim // Q_CHUNK,)), pltpu.SemaphoreType.DMA((n_tok // TOK_STEP,)), pltpu.SemaphoreType.DMA((n_tok // TOK_STEP,)),
                ],
                compiler_params=pltpu.CompilerParams(vmem_limit_bytes=VMEM_BYTES),
            )(cache_len, x_cur, row_len, ids_t, router_t, w_query, w_key, w_value, w_out, k_rows, v_rows)
            x_cur = pl.pallas_call(
                functools.partial(moe_kernel, layer, capacity, ep_size),
                name=f"moe_{layer}",
                out_shape=jax.ShapeDtypeStruct((n_tok, d_model), BF16),
                in_specs=[ANY] * 9,
                out_specs=VMEM,
                scratch_shapes=[
                    pltpu.VMEM((n_tok, ext), BF16), pltpu.VMEM((n_tok, d_model), BF16), pltpu.VMEM((n_tok, META), F32),
                    pltpu.VMEM((ep_size, n_tok, ext), BF16), pltpu.VMEM((ep_size, capacity, d_model), BF16),
                    pltpu.VMEM((n_rows, d_model), BF16), pltpu.VMEM((ep_size, capacity, d_model), BF16),
                    pltpu.VMEM((n_rows, d_model), F32), pltpu.VMEM((CHIP_CORES * n_tok, d_model), F32),
                    pltpu.VMEM((CHIP_CORES * n_tok, d_model), BF16), pltpu.VMEM((n_tok, d_model), F32),
                    pltpu.VMEM(w_gate.shape[2:], BF16), pltpu.VMEM(w_up.shape[2:], BF16), pltpu.VMEM(w_down.shape[2:], BF16),
                    pltpu.VMEM((SHARED_RING, d_model, SHARED_CHUNK), BF16), pltpu.VMEM((SHARED_RING, d_model, SHARED_CHUNK), BF16), pltpu.VMEM((SHARED_RING, SHARED_CHUNK, d_model), BF16),
                    pltpu.SemaphoreType.DMA((w_gate.shape[3] // FF_CHUNK, 3)), pltpu.SemaphoreType.DMA((SHARED_RING, 3)), pltpu.SemaphoreType.DMA((14,)), pltpu.SemaphoreType.DMA((ep_size, 2)),
                    pltpu.SemaphoreType.DMA((ep_size,)), pltpu.SemaphoreType.DMA((ep_size,)), pltpu.SemaphoreType.DMA, pltpu.SemaphoreType.DMA, pltpu.SemaphoreType.DMA((3,)),
                ],
                compiler_params=pltpu.CompilerParams(vmem_limit_bytes=VMEM_BYTES, collective_id=layer, has_side_effects=True),
            )(u_ext, resid, meta, shared_gate, shared_up, shared_down, w_gate, w_up, w_down)
        return x_cur

    return jax.shard_map(body, mesh=mesh, in_specs=in_specs, out_specs=row_spec, check_vma=False)
```

```python
import functools
import math
import jax
import jax.numpy as jnp
from jax import lax
from jax.experimental import pallas as pl
from jax.experimental.pallas import tpu as pltpu
from jax.sharding import PartitionSpec as P

RMS_EPS = 1e-6
ROPE_BASE = 10000.0
MESH = pl.DeviceIdType.MESH
BF16 = jnp.bfloat16
F32 = jnp.float32
ANY = pl.BlockSpec(memory_space=pl.ANY)
VMEM = pl.BlockSpec(memory_space=pltpu.VMEM)
SMEM = pl.BlockSpec(memory_space=pltpu.SMEM)
VMEM_BYTES = 66_000_000
META = 128
TOK_STEP = 16
FF_CHUNK = 512
LOOKAHEAD = 3
OWN_FIRST = 5
PASS_CHUNK = 2048
SHARED_CHUNK = 512
SHARED_RING = 2
Q_CHUNK = 512
CHIP_CORES = 2
ROW_TILE = 128


def rms(vals):
    return vals * lax.rsqrt(jnp.mean(vals * vals, axis=-1, keepdims=True) + RMS_EPS)


def mm(lhs, rhs):
    return jnp.dot(lhs, rhs, preferred_element_type=F32)


def silu(vals):
    return vals * (1.0 / (1.0 + jnp.exp(-vals)))


def attention_kernel(layer, capacity, q_heads, kv_heads, lens, x_ref, row_len_ref, ids_ref, wr_ref, wq, wk, wv, wo, kc, vc,
                     a_ref, u_ref, meta_ref, x_v, wr_v, wr_parts, wq_b, wk_b, wv_b, wo_b, k_b, v_b, q3, kn3, vn3, o3, attn, in_sem, w_sem, q_sem, k_sem, v_sem):
    n_tok, d_model = x_ref.shape
    rows = kc.shape[2]
    head_dim = kc.shape[3]
    group = q_heads // kv_heads
    steps = n_tok // TOK_STEP
    q_steps = q_heads * head_dim // Q_CHUNK
    first = lax.axis_index("pool") * n_tok
    scale = head_dim ** -0.5
    k_copy = pltpu.make_async_copy(wk.at[layer], wk_b, w_sem.at[0])
    v_copy = pltpu.make_async_copy(wv.at[layer], wv_b, w_sem.at[1])
    o_copy = pltpu.make_async_copy(wo.at[layer], wo_b, w_sem.at[2])

    def q_copy(step):
        cols = pl.ds(step * Q_CHUNK, Q_CHUNK)
        return pltpu.make_async_copy(wq.at[layer, :, cols], wq_b.at[:, cols], q_sem.at[step])

    def cache_copies(step):
        here = pl.ds(step * TOK_STEP, TOK_STEP)
        there = pl.ds(first + step * TOK_STEP, TOK_STEP)
        return (pltpu.make_async_copy(kc.at[layer, there], k_b.at[here], k_sem.at[step]),
                pltpu.make_async_copy(vc.at[layer, there], v_b.at[here], v_sem.at[step]))

    def start_cache(step):
        for copy in cache_copies(step):
            copy.start()

    x_copy = pltpu.make_async_copy(x_ref, x_v, in_sem.at[0])
    wr_copy = pltpu.make_async_copy(wr_ref.at[layer], wr_v, in_sem.at[1])
    x_copy.start()
    wr_copy.start()
    k_copy.start()
    v_copy.start()
    q_copy(0).start()

    q3[:, q_heads:, :] = jnp.zeros((n_tok, q3.shape[1] - q_heads, head_dim), F32)
    kn3[:, q_heads:, :] = jnp.zeros((n_tok, q3.shape[1] - q_heads, head_dim), F32)
    vn3[:, q_heads:, :] = jnp.zeros((n_tok, q3.shape[1] - q_heads, head_dim), F32)
    experts = wr_v.shape[0]
    all_tok = row_len_ref.shape[1]
    mine = lax.broadcasted_iota(jnp.int32, (n_tok, all_tok), 1) == first + lax.broadcasted_iota(jnp.int32, (n_tok, all_tok), 0)

    def column(row):
        return jnp.sum(jnp.where(mine, row.astype(F32), 0.0), axis=-1, keepdims=True)

    x_copy.wait()
    x_f = x_v[...].astype(F32)
    hidden = rms(x_f).astype(BF16)
    lane_d = lax.broadcasted_iota(jnp.int32, (n_tok, head_dim), 1)
    half = head_dim // 2
    inv_freq = jnp.exp(lax.rem(lane_d, half).astype(F32) * (-math.log(ROPE_BASE) / half))
    angle = column(row_len_ref[...]) * inv_freq
    cosine = jnp.cos(angle)
    sine = jnp.sin(angle)
    sine = jnp.where(lane_d < half, -sine, sine)

    def rotated(vals):
        return (vals * cosine + pltpu.roll(vals, half, 1) * sine).astype(BF16).astype(F32)

    wr_copy.wait()
    coarse = wr_v[...].astype(BF16)
    rest = wr_v[...] - coarse.astype(F32)
    middle = rest.astype(BF16)
    fine = (rest - middle.astype(F32)).astype(BF16)
    wr_parts[0:experts] = coarse.astype(F32)
    wr_parts[experts:2 * experts] = middle.astype(F32)
    wr_parts[2 * experts:3 * experts] = fine.astype(F32)
    k_copy.wait()
    q_copy(1).start()
    key = mm(hidden, wk_b[...])
    v_copy.wait()
    q_copy(2).start()
    val = mm(hidden, wv_b[...]).astype(BF16).astype(F32)
    for kv in range(kv_heads):
        cols = slice(kv * head_dim, (kv + 1) * head_dim)
        key_rot = rotated(key[:, cols])
        for head in range(kv * group, (kv + 1) * group):
            kn3[:, head, :] = key_rot
            vn3[:, head, :] = val[:, cols]
    for step in range(q_steps):
        q_copy(step).wait()
        start_cache(step)
        query = mm(hidden, wq_b[:, step * Q_CHUNK:(step + 1) * Q_CHUNK])
        for i in range(Q_CHUNK // head_dim):
            q3[:, step * (Q_CHUNK // head_dim) + i, :] = rotated(query[:, i * head_dim:(i + 1) * head_dim])
    for step in range(q_steps, steps):
        start_cache(step)
    o_copy.start()

    pad = q3.shape[1]
    lane = lax.broadcasted_iota(jnp.int32, (pad, rows), 1)
    head_kv = lax.broadcasted_iota(jnp.int32, (pad, rows), 0) // group
    right_kv = lane % kv_heads == head_kv
    position = lane // kv_heads

    def step_body(step, carry):
        for copy in cache_copies(step):
            copy.wait()
        base = step * TOK_STEP
        q_f = q3[pl.ds(base, TOK_STEP)]
        scores = lax.dot_general(q_f.astype(BF16), k_b[pl.ds(base, TOK_STEP)], (((2,), (2,)), ((0,), (0,))), preferred_element_type=F32)
        s_new = jnp.sum(q_f * kn3[pl.ds(base, TOK_STEP)], axis=-1, keepdims=True) * scale
        probs = []
        p_news = []
        for i in range(TOK_STEP):
            valid = right_kv & (position < lens[first + base + i])
            s_i = jnp.where(valid, scores[i] * scale, -jnp.inf)
            peak = jnp.maximum(jnp.max(s_i, axis=-1, keepdims=True), s_new[i])
            e_i = jnp.exp(s_i - peak)
            e_new = jnp.exp(s_new[i] - peak)
            total = jnp.sum(e_i, axis=-1, keepdims=True) + e_new
            probs.append((e_i / total).astype(BF16))
            p_news.append((e_new / total).astype(BF16).astype(F32))
        for i in range(TOK_STEP):
            mixed = mm(probs[i], v_b[base + i])
            o3[base + i] = mixed + p_news[i] * vn3[base + i]
        return carry

    lax.fori_loop(0, steps, step_body, 0)
    for head in range(q_heads):
        attn[:, head * head_dim:(head + 1) * head_dim] = o3[:, head, :].astype(BF16)
    o_copy.wait()
    resid = (x_f + mm(attn[...], wo_b[...])).astype(BF16)
    a_ref[...] = resid
    normed = rms(resid.astype(F32)).astype(BF16)
    u_ref[:, :d_model] = normed

    logits = lax.dot_general(normed, wr_parts[...].astype(BF16), (((1,), (1,)), ((), ())), preferred_element_type=F32)
    column_id = lax.broadcasted_iota(jnp.int32, logits.shape, 1)
    column_id = lax.rem(column_id, experts).astype(F32)
    lane_e = lax.broadcasted_iota(jnp.int32, (n_tok, META), 1).astype(F32)
    id0 = column(ids_ref[layer, 0:1, :])
    id1 = column(ids_ref[layer, 1:2, :])
    pick0 = lane_e == id0
    pick1 = lane_e == id1
    l0 = jnp.sum(jnp.where(column_id == id0, logits, 0.0), axis=-1, keepdims=True)
    l1 = jnp.sum(jnp.where(column_id == id1, logits, 0.0), axis=-1, keepdims=True)
    peak = jnp.maximum(l0, l1)
    e0 = jnp.exp(l0 - peak)
    e1 = jnp.exp(l1 - peak)
    member = jnp.where(pick0 | pick1, 1.0, 0.0)
    earlier = jnp.where(lax.broadcasted_iota(jnp.int32, (n_tok, n_tok), 1) < lax.broadcasted_iota(jnp.int32, (n_tok, n_tok), 0), 1.0, 0.0)
    rank = mm(earlier.astype(BF16), member.astype(BF16))
    u_ref[:, d_model:] = jnp.where(member > 0.0, rank, -1.0).astype(BF16)
    slot0 = id0 * capacity + jnp.sum(jnp.where(pick0, rank, 0.0), axis=-1, keepdims=True)
    slot1 = id1 * capacity + jnp.sum(jnp.where(pick1, rank, 0.0), axis=-1, keepdims=True)
    total = e0 + e1
    meta_ref[...] = jnp.where(lane_e == 0, slot0, jnp.where(lane_e == 1, slot1, jnp.where(lane_e == 2, e0 / total, e1 / total)))


def row_blocks(capacity, blocks=((0, 2), (2, 4), (4, 8))):
    sizes = [-(-(hi - lo) * capacity // ROW_TILE) * ROW_TILE if (hi - lo) * capacity < ROW_TILE else (hi - lo) * capacity for lo, hi in blocks]
    return [sum(sizes[:i]) for i in range(len(sizes))], sizes


def moe_kernel(layer, capacity, ep_size, u_ref, a_ref, meta_ref, sg, su, sd, wg, wu, wd, out_ref,
               gath, back, picked, sent, acc_e, acc_s, pair, other_s, g_w, u_w, d_w, g_b, u_b, d_b, e_sem, s_sem, ag_send, ag_recv, ret_send, ret_recv, sum_send, sum_recv):
    n_tok = a_ref.shape[0]
    d_model = a_ref.shape[1]
    half = n_tok // 2
    e_chunks = wg.shape[3] // FF_CHUNK
    s_chunks = sg.shape[2] // (SHARED_CHUNK * CHIP_CORES)
    me = lax.axis_index("ep")
    partner = me + 1 - 2 * lax.rem(me, 2)
    right = lax.rem(me + 2, ep_size)
    left = lax.rem(me + ep_size - 2, ep_size)
    far = lax.rem(me + ep_size // 2, ep_size)
    p_right = lax.rem(partner + 2, ep_size)
    p_left = lax.rem(partner + ep_size - 2, ep_size)
    p_far = lax.rem(partner + ep_size // 2, ep_size)
    places = [me, partner, far, p_far, right, p_right, left, p_left]
    blocks = [(0, 2), (2, 4), (4, 8)]
    starts, sizes = row_blocks(capacity, blocks)
    row_of = {place: starts[i] + (place - lo) * capacity for i, (lo, hi) in enumerate(blocks) for place in range(lo, hi)}

    def expert_copies(chunk):
        cols = pl.ds(chunk * FF_CHUNK, FF_CHUNK)
        pairs = ((wg.at[layer, 0, :, cols], g_w.at[:, cols]), (wu.at[layer, 0, :, cols], u_w.at[:, cols]), (wd.at[layer, 0, cols], d_w.at[cols]))
        return [pltpu.make_async_copy(src, dst, e_sem.at[chunk, i]) for i, (src, dst) in enumerate(pairs)]

    s_first = lax.rem(me, CHIP_CORES) * s_chunks

    def shared_copies(chunk, slot):
        cols = pl.ds((s_first + chunk) * SHARED_CHUNK, SHARED_CHUNK)
        pairs = ((sg.at[layer, :, cols], g_b.at[slot]), (su.at[layer, :, cols], u_b.at[slot]), (sd.at[layer, cols], d_b.at[slot]))
        return [pltpu.make_async_copy(src, dst, s_sem.at[slot, i]) for i, (src, dst) in enumerate(pairs)]

    for chunk in range(LOOKAHEAD):
        for copy in expert_copies(chunk):
            copy.start()

    barrier = pltpu.get_barrier_semaphore()
    for other in range(1, ep_size):
        pl.semaphore_signal(barrier, inc=1, device_id={"ep": lax.rem(me + other, ep_size)}, device_id_type=MESH)
    gath[me] = u_ref[...]
    pl.semaphore_wait(barrier, ep_size - 1)

    def piece(src, part):
        return gath.at[src, pl.ds(part * half, half)]

    def arrived(src, part):
        pltpu.make_async_remote_copy(src_ref=piece(src, part), dst_ref=piece(src, part), send_sem=ag_send.at[0], recv_sem=ag_recv.at[src, part],
                                     device_id={"ep": partner}, device_id_type=MESH).wait_recv()

    sends = []

    def send(src, part, target, from_input=False):
        ref = u_ref.at[pl.ds(part * half, half)] if from_input else piece(src, part)
        copy = pltpu.make_async_remote_copy(src_ref=ref, dst_ref=piece(src, part), send_sem=ag_send.at[len(sends)], recv_sem=ag_recv.at[src, part],
                                            device_id={"ep": target}, device_id_type=MESH)
        copy.start()
        sends.append(copy)

    send(me, 0, partner, True)
    send(me, 1, partner, True)
    send(me, 0, right, True)
    send(me, 1, left, True)
    send(me, 1, right, True)
    send(me, 0, left, True)

    acc_s[...] = jnp.zeros_like(acc_s)
    acc_e[...] = jnp.zeros_like(acc_e)
    picked[...] = jnp.zeros_like(picked)
    lane = lax.broadcasted_iota(jnp.int32, (n_tok, META), 1)

    def pick(src, codes, values, place):
        rank = jnp.sum(jnp.where(lane == me, codes.astype(F32), 0.0), axis=-1, keepdims=True)
        choose = jnp.where(lane.astype(F32) == rank, 1.0, 0.0).astype(BF16)
        rows = lax.dot_general(choose, values, (((0,), (0,)), ((), ())), preferred_element_type=F32)
        picked[pl.ds(row_of[place], capacity)] = rows[:capacity].astype(BF16)

    def pick_places(first, last):
        for place in range(first, last):
            src = places[place]
            if place == 0:
                pick(src, u_ref[:, d_model:], u_ref[:, :d_model], place)
            else:
                pick(src, gath[src, :, d_model:], gath[src, :, :d_model], place)

    def expert_rows(block, chunk, width):
        rows = pl.ds(starts[block], sizes[block])
        cols = pl.ds(pl.multiple_of(chunk * width, width), width)
        x_rows = picked[rows]
        mid = (silu(mm(x_rows, g_w[:, cols])) * mm(x_rows, u_w[:, cols])).astype(BF16)
        acc_e[rows] += mm(mid, d_w[cols])

    def return_copy(place):
        target = places[place]
        return pltpu.make_async_remote_copy(src_ref=sent.at[place], dst_ref=back.at[me], send_sem=ret_send.at[place], recv_sem=ret_recv.at[me],
                                            device_id={"ep": target}, device_id_type=MESH)

    def give_back(first, last):
        for place in range(first, last):
            sent[place] = acc_e[pl.ds(row_of[place], capacity)].astype(BF16)
        for place in range(max(first, 1), last):
            return_copy(place).start()

    def own_step(chunk, carry):
        for copy in expert_copies(chunk):
            copy.wait()

        @pl.when(chunk + LOOKAHEAD < e_chunks)
        def _():
            for copy in expert_copies(chunk + LOOKAHEAD):
                copy.start()

        expert_rows(0, chunk, FF_CHUNK)
        return carry

    for part in (0, 1):
        arrived(partner, part)
    pick_places(0, 2)
    lax.fori_loop(0, 2, own_step, 0)
    arrived(left, 0)
    send(left, 0, right)
    arrived(right, 1)
    send(right, 1, left)
    send(left, 0, partner)
    send(right, 1, partner)
    lax.fori_loop(2, 4, own_step, 0)
    for src, part in ((left, 1), (right, 0)):
        arrived(src, part)
        send(src, part, partner)
    lax.fori_loop(4, OWN_FIRST, own_step, 0)
    for slot in range(SHARED_RING):
        for copy in shared_copies(slot, slot):
            copy.start()
    for src in (p_right, p_left):
        for part in (0, 1):
            arrived(src, part)
    pick_places(4, 8)
    per_step = PASS_CHUNK // FF_CHUNK
    sent_before = len(sends)

    def far_copy(part):
        return pltpu.make_async_remote_copy(src_ref=piece(far, part), dst_ref=piece(far, part), send_sem=ag_send.at[sent_before + part],
                                            recv_sem=ag_recv.at[far, part], device_id={"ep": partner}, device_id_type=MESH)


    def near_step(step, carry):
        for chunk in range(OWN_FIRST, e_chunks):

            @pl.when(step == chunk // per_step)
            def _():
                for copy in expert_copies(chunk):
                    copy.wait()

        expert_rows(2, step, PASS_CHUNK)

        @pl.when(step == 0)
        def _():
            for part in (0, 1):
                arrived(far, part)
                far_copy(part).start()

        return carry

    lax.fori_loop(0, e_chunks // per_step, near_step, 0)
    give_back(4, 8)
    for src in (p_far,):
        for part in (0, 1):
            arrived(src, part)
    pick_places(2, 4)

    def far_step(step, carry):
        expert_rows(1, step, PASS_CHUNK)
        return carry

    lax.fori_loop(0, e_chunks // per_step, far_step, 0)
    give_back(2, 4)

    def own_rest(chunk, carry):
        expert_rows(0, chunk, FF_CHUNK)
        return carry

    lax.fori_loop(OWN_FIRST, e_chunks, own_rest, 0)
    give_back(0, 2)
    pair[pl.ds(0, n_tok)] = u_ref[:, :d_model]
    pair[pl.ds(n_tok, n_tok)] = gath[partner, :, :d_model]

    def shared_step(chunk, carry):
        slot = lax.rem(chunk, SHARED_RING)
        for copy in shared_copies(chunk, slot):
            copy.wait()
        rows = pair[...]
        mid = (silu(mm(rows, g_b[slot])) * mm(rows, u_b[slot])).astype(BF16)
        acc_s[...] += mm(mid, d_b[slot])

        @pl.when(chunk + SHARED_RING < s_chunks)
        def _():
            for copy in shared_copies(chunk + SHARED_RING, slot):
                copy.start()

        return carry

    lax.fori_loop(0, s_chunks, shared_step, 0)
    sum_copy = pltpu.make_async_remote_copy(src_ref=acc_s.at[pl.ds(n_tok, n_tok)], dst_ref=other_s, send_sem=sum_send, recv_sem=sum_recv,
                                            device_id={"ep": partner}, device_id_type=MESH)
    sum_copy.start()
    back[me] = sent[0]
    for copy in sends + [far_copy(0), far_copy(1)]:
        copy.wait_send()
    for place in range(1, ep_size):
        return_copy(place).wait_send()
        src = places[place]
        pltpu.make_async_remote_copy(src_ref=back.at[src], dst_ref=back.at[src], send_sem=ret_send.at[place], recv_sem=ret_recv.at[src],
                                     device_id={"ep": src}, device_id_type=MESH).wait_recv()

    slot_lane = lax.broadcasted_iota(jnp.int32, (n_tok, ep_size * capacity), 1).astype(F32)
    table = back[...].reshape(ep_size * capacity, d_model)
    choose = jnp.concatenate([jnp.where(slot_lane == meta_ref[:, 0:1], 1.0, 0.0), jnp.where(slot_lane == meta_ref[:, 1:2], 1.0, 0.0)], axis=0).astype(BF16)
    y_pair = mm(choose, table)
    routed = meta_ref[:, 2:3] * y_pair[:n_tok] + meta_ref[:, 3:4] * y_pair[n_tok:]
    sum_copy.wait()
    shared_out = (acc_s[pl.ds(0, n_tok)] + other_s[...]).astype(BF16).astype(F32)
    out_ref[...] = (a_ref[...].astype(F32) + routed + shared_out).astype(BF16)


def solution(mesh):
    ep_size = mesh.shape["ep"]
    row_spec = P(("dp", "ep", "pool"), None)
    cache_spec = P(None, ("dp", "ep"), None, None, None)
    expert_spec = P(None, "ep", None, None)
    in_specs = (row_spec, cache_spec, cache_spec, P(("dp", "ep")), P(), P(), P(), P(), P(), P(None, ("dp", "ep"), None), expert_spec, expert_spec, expert_spec, P(), P(), P())

    def body(x_loc, k_cache, v_cache, cache_len, w_query, w_key, w_value, w_out, w_router, expert_ids, w_gate, w_up, w_down, shared_gate, shared_up, shared_down):
        n_tok, d_model = x_loc.shape
        n_layers, all_tok, ctx, kv_heads, head_dim = k_cache.shape
        q_heads = w_query.shape[2] // head_dim
        top_k = expert_ids.shape[2]
        capacity = 3 * n_tok * top_k // ep_size
        rows = ctx * kv_heads
        pad_heads = -(-q_heads // 8) * 8
        ids_t = jnp.swapaxes(expert_ids, 1, 2)
        row_len = cache_len.reshape(1, cache_len.shape[0])
        router_t = jnp.swapaxes(w_router, 1, 2)
        k_rows = k_cache.reshape(n_layers, all_tok, rows, head_dim)
        v_rows = v_cache.reshape(n_layers, all_tok, rows, head_dim)
        ext = d_model + META
        n_rows = sum(row_blocks(capacity)[1])
        x_cur = x_loc
        for layer in range(n_layers):
            resid, u_ext, meta = pl.pallas_call(
                functools.partial(attention_kernel, layer, capacity, q_heads, kv_heads),
                name=f"attention_{layer}",
                out_shape=(jax.ShapeDtypeStruct((n_tok, d_model), BF16), jax.ShapeDtypeStruct((n_tok, ext), BF16), jax.ShapeDtypeStruct((n_tok, META), F32)),
                in_specs=[SMEM, ANY, VMEM, VMEM] + [ANY] * 7,
                out_specs=(VMEM, VMEM, VMEM),
                scratch_shapes=[
                    pltpu.VMEM((n_tok, d_model), BF16), pltpu.VMEM(router_t.shape[1:], F32), pltpu.VMEM((3 * router_t.shape[1], d_model), F32),
                    pltpu.VMEM(w_query.shape[1:], BF16), pltpu.VMEM(w_key.shape[1:], BF16), pltpu.VMEM(w_value.shape[1:], BF16), pltpu.VMEM(w_out.shape[1:], BF16),
                    pltpu.VMEM((n_tok, rows, head_dim), BF16), pltpu.VMEM((n_tok, rows, head_dim), BF16),
                    pltpu.VMEM((n_tok, pad_heads, head_dim), F32), pltpu.VMEM((n_tok, pad_heads, head_dim), F32),
                    pltpu.VMEM((n_tok, pad_heads, head_dim), F32), pltpu.VMEM((n_tok, pad_heads, head_dim), F32),
                    pltpu.VMEM((n_tok, q_heads * head_dim), BF16),
                    pltpu.SemaphoreType.DMA((2,)), pltpu.SemaphoreType.DMA((3,)), pltpu.SemaphoreType.DMA((q_heads * head_dim // Q_CHUNK,)), pltpu.SemaphoreType.DMA((n_tok // TOK_STEP,)), pltpu.SemaphoreType.DMA((n_tok // TOK_STEP,)),
                ],
                compiler_params=pltpu.CompilerParams(vmem_limit_bytes=VMEM_BYTES),
            )(cache_len, x_cur, row_len, ids_t, router_t, w_query, w_key, w_value, w_out, k_rows, v_rows)
            x_cur = pl.pallas_call(
                functools.partial(moe_kernel, layer, capacity, ep_size),
                name=f"moe_{layer}",
                out_shape=jax.ShapeDtypeStruct((n_tok, d_model), BF16),
                in_specs=[VMEM] * 3 + [ANY] * 6,
                out_specs=VMEM,
                scratch_shapes=[
                    pltpu.VMEM((ep_size, n_tok, ext), BF16), pltpu.VMEM((ep_size, capacity, d_model), BF16),
                    pltpu.VMEM((n_rows, d_model), BF16), pltpu.VMEM((ep_size, capacity, d_model), BF16),
                    pltpu.VMEM((n_rows, d_model), F32), pltpu.VMEM((CHIP_CORES * n_tok, d_model), F32),
                    pltpu.VMEM((CHIP_CORES * n_tok, d_model), BF16), pltpu.VMEM((n_tok, d_model), F32),
                    pltpu.VMEM(w_gate.shape[2:], BF16), pltpu.VMEM(w_up.shape[2:], BF16), pltpu.VMEM(w_down.shape[2:], BF16),
                    pltpu.VMEM((SHARED_RING, d_model, SHARED_CHUNK), BF16), pltpu.VMEM((SHARED_RING, d_model, SHARED_CHUNK), BF16), pltpu.VMEM((SHARED_RING, SHARED_CHUNK, d_model), BF16),
                    pltpu.SemaphoreType.DMA((w_gate.shape[3] // FF_CHUNK, 3)), pltpu.SemaphoreType.DMA((SHARED_RING, 3)), pltpu.SemaphoreType.DMA((14,)), pltpu.SemaphoreType.DMA((ep_size, 2)),
                    pltpu.SemaphoreType.DMA((ep_size,)), pltpu.SemaphoreType.DMA((ep_size,)), pltpu.SemaphoreType.DMA, pltpu.SemaphoreType.DMA,
                ],
                compiler_params=pltpu.CompilerParams(vmem_limit_bytes=VMEM_BYTES, collective_id=layer, has_side_effects=True),
            )(u_ext, resid, meta, shared_gate, shared_up, shared_down, w_gate, w_up, w_down)
        return x_cur

    return jax.shard_map(body, mesh=mesh, in_specs=in_specs, out_specs=row_spec, check_vma=False)
```
